128 devices in a mesh: ep: 128 (over y, z, x, core).
Axes of the slice: x: 4, y: 4, z: 4, core: 2. Of those that a mesh axis runs over, the one named last changes fastest.
Arguments:
- tokens: bfloat16 [16384, 7168], P('ep'), may hold values from -6 to 6
- expert_ids: int32 [16384, 8], P('ep'), may hold values from 0 to 255, all different within a row; in each aligned block of 128 rows (0 to 127, 128 to 255, ...) at most 6 rows name the same one
Outputs:
- merged: bfloat16 [256, 768, 7168], P('ep')
- totals: int32 [256], P('ep')
The draws below stay inside these ranges and needn't reach their ends.
Inputs may be any that keep to these rules, and one draw needn't show every extreme that they name: `expert_ids`: each row names 8 different experts; among the rows of one device (aligned blocks of 128 rows) no expert is named more than 6 times, a bound that some block reaches.
All inputs are finite; a program needn't handle non-finite values.
Results may differ from the reference program's by a relative error of at most 0.001.
Values may be sent and summed in bfloat16 or wider, within the bound.
A program may use at most 256 MiB of HBM per device.

```python
import math
import jax
import jax.numpy as jnp
import numpy as np
from jax import lax

D = 7168
EXPERTS = 256
TOP = 8
TOK_DEV = 128
CAP = 6
TOKENS = 16384
N_EP = 128


def block_levels(own_key, extent, cuts, low, high):
    loudness = 1.0
    for dim, shards_of in cuts:
        steps = jax.random.uniform(jax.random.fold_in(jax.random.fold_in(own_key, 6), dim), (shards_of,), jnp.float32, low / len(cuts), high / len(cuts))
        loudness = loudness * jnp.repeat(jnp.exp(steps), extent[dim] // shards_of).reshape((-1,) + (1,) * (len(extent) - 1 - dim))
    return loudness


def deal_out(stream_key, own, number, rows, count, top, bound, skew):
    sequence = jax.random.permutation(stream_key, count)
    heavy_load, common = shares(count, rows * top, bound, skew, True), shares(count, rows * top, bound, skew, False)
    places = jnp.arange(count)

    def named(tallies, offset_by):
        used = int((tallies > 0).sum())
        fixed = max(1, used // 4)
        shifted = fixed + (places - fixed + offset_by * (used - fixed)) % max(1, count - fixed)
        return jnp.zeros((count,), jnp.int32).at[sequence[jnp.where(places < fixed, places, shifted)]].set(jnp.asarray(tallies, jnp.int32))

    tallies = jnp.where(number % 4 == 0, named(heavy_load, number // 4), named(common, number - number // 4 - 1))
    mixed = jax.random.permutation(jax.random.fold_in(own, 3), count)
    source_of, receiver = mixed[0:count // 2 * 2:2], mixed[1:count // 2 * 2:2]
    slack = jnp.minimum(tallies[source_of] - 1, bound - tallies[receiver]) // 2
    slack = jnp.where((source_of == sequence[0]) | (receiver == sequence[0]) | (tallies[receiver] == 0), 0, jnp.maximum(slack, 0))
    shifted = jax.random.randint(jax.random.fold_in(own, 4), (count // 2,), 0, 1 << 20) % (slack + 1)
    tallies = tallies.at[source_of].add(-shifted).at[receiver].add(shifted)
    members = jnp.searchsorted(jnp.cumsum(tallies), jnp.arange(rows * top), side="right").astype(jnp.int32)
    listing = members.reshape(top, rows).T
    listing = listing[jax.random.permutation(jax.random.fold_in(own, 1), rows)]
    offset_by = jax.random.randint(jax.random.fold_in(own, 2), (rows, 1), 0, top)
    return jnp.take_along_axis(listing, (jnp.arange(top)[None, :] + offset_by) % top, axis=1)


def shares(number_of, total, most, skew, full):
    loads = [(1 << 20) // math.isqrt(grade ** skew) + 1 for grade in range(1, number_of + 1)]
    largest = most if full else min(most, max(-(-total // number_of), total * loads[0] // sum(loads)))
    least = 1 if total - largest >= number_of - 1 else 0
    counts, surplus = [largest] + [least] * (number_of - 1), total - largest - least * (number_of - 1)
    while surplus > 0:
        free = [i for i in range(1, number_of) if counts[i] < largest] or [i for i in range(1, number_of) if counts[i] < most]
        pool, budget = sum([loads[i] for i in free]), surplus
        for i in free:
            extra = min(most - counts[i], max(1, budget * loads[i] // pool), surplus)
            counts[i] = counts[i] + extra
            surplus = surplus - extra
    return np.array(counts)


def gaussian(key, shape, width, most, pieces=(), kind=jnp.bfloat16):
    result = jax.random.normal(key, shape, jnp.float32) * width
    if len(pieces) > 0:
        result = block_levels(key, shape, pieces, -0.22, 0.18) * result
    return jnp.clip(result, min=-most, max=most).astype(kind)


def setup_inputs(seed: int = 0) -> dict:
    arg_keys = jax.random.split(jax.random.key(seed), 3)
    tokens = gaussian(arg_keys[0], (TOKENS, D), 1.0, 6.0, ((0, 128),))
    expert_ids_keys = jax.random.split(jax.random.fold_in(arg_keys[1], 1), TOKENS // TOK_DEV)
    expert_ids_turns = jax.random.permutation(jax.random.fold_in(arg_keys[1], 3), TOKENS // TOK_DEV)
    expert_ids = jax.vmap(lambda own, number: deal_out(jax.random.fold_in(arg_keys[1], 2), own, number, TOK_DEV, EXPERTS, TOP, CAP, 2))(expert_ids_keys, expert_ids_turns).reshape((TOKENS, TOP))
    return {"tokens": tokens, "expert_ids": expert_ids}


def reference(tokens, expert_ids):
    lines = N_EP * CAP
    count_tokens = tokens.shape[0]

    def one_expert(expert):
        mark = jnp.sum((expert_ids == expert).astype(jnp.int32), axis=1).astype(jnp.int32)
        running = jnp.cumsum(mark).astype(jnp.int32)
        total = running[count_tokens - 1]
        wanted = jnp.arange(lines, dtype=jnp.int32) + 1
        source = jnp.searchsorted(running, wanted).astype(jnp.int32)
        source = jnp.minimum(source, count_tokens - 1).astype(jnp.int32)
        picked = jnp.take(tokens, source, axis=0)
        keep = (wanted <= total)[:, None]
        return jnp.where(keep, picked, jnp.zeros_like(picked)), total

    merged, totals = lax.map(one_expert, jnp.arange(EXPERTS, dtype=jnp.int32))
    return merged, totals.astype(jnp.int32)
```

```python
import functools

import jax
import jax.numpy as jnp
from jax import lax
from jax.experimental import pallas as pl
from jax.experimental.pallas import tpu as pltpu
from jax.sharding import PartitionSpec as P

EXPERTS = 256
CAP = 6
TOP = 8
TOK = 128
WIDTH = 7168
HALF = WIDTH // 2
QUARTER = HALF // 2
PIECE = QUARTER // 2
LINES = 768
SPLITS = ((0, 640), (640, 640), (1280, 512))
MESH = pl.DeviceIdType.MESH


def near(v):
    return v + 1 - 2 * (v % 2)


def far(v):
    return 3 - v


SHARE = (near, far)
CROSS = (far, near)
PAIR = (lambda v: v // 2, lambda v: ((v + 1) // 2) % 2)
MEMBER = (lambda v: v % 2, lambda v: v // 2)
ORDER = (None, (0, 3, 1, 2))


def pick(flag, flipped, value):
    return value + flag * (flipped - value)


def exchange(tok, ids, out, xg, oh, sb, mk, rk, load_sem, swap_send, swap_recv,
             ag_send, ag_recv, put_send, put_recv, keep_sem):
    me = lax.axis_index("ep")
    core, x, z, y = me % 2, (me // 2) % 4, (me // 8) % 4, me // 32

    def device(yy, zz, xx, cc):
        return ((yy * 4 + zz) * 4 + xx) * 2 + cc

    def target(h, d):
        flip = CROSS[h]
        return device(
            pick(d // 8, flip(y), y),
            pick((d // 4) % 2, flip(z), z),
            pick((d // 2) % 2, flip(x), x),
            pick(d % 2, 1 - core, core),
        )

    loads = []
    for h in range(2):
        copy = pltpu.make_async_copy(
            tok.at[:, pl.ds(pl.multiple_of(h * HALF + core * QUARTER, 128), QUARTER)],
            xg.at[h, 0, pl.ds(pl.multiple_of(core * TOK, TOK), TOK), :],
            load_sem.at[h],
        )
        copy.start()
        loads.append(copy)

    barrier = pltpu.get_barrier_semaphore()
    for h in range(2):
        for d in range(1, 16):
            if h == 0 or d >= 2:
                pl.semaphore_signal(barrier, inc=1, device_id=(target(h, d),), device_id_type=MESH)
    pl.semaphore_wait(barrier, 29)

    partner = device(y, z, x, 1 - core)
    swaps = []
    for h in range(2):
        copy = pltpu.make_async_remote_copy(
            src_ref=tok.at[:, pl.ds(pl.multiple_of(h * HALF + (1 - core) * QUARTER, 128), QUARTER)],
            dst_ref=xg.at[h, 0, pl.ds(pl.multiple_of(core * TOK, TOK), TOK), :],
            send_sem=swap_send.at[h],
            recv_sem=swap_recv.at[h],
            device_id=(partner,),
            device_id_type=MESH,
        )
        copy.start()
        swaps.append(copy)

    def neighbour(h, bit):
        flip = SHARE[h]
        if bit == 1:
            return device(y, z, flip(x), core)
        if bit == 2:
            return device(y, flip(z), x, core)
        return device(flip(y), z, x, core)

    def spread(h, i, slot, bit):
        at, size = SPLITS[i]
        return pltpu.make_async_remote_copy(
            src_ref=xg.at[h, slot, :, pl.ds(at, size)],
            dst_ref=xg.at[h, slot ^ bit, :, pl.ds(at, size)],
            send_sem=ag_send.at[h, i, slot ^ bit],
            recv_sem=ag_recv.at[h, i, slot ^ bit],
            device_id=(neighbour(h, bit),),
            device_id_type=MESH,
        )

    def step_slots(i, step):
        bits = [(1, 2, 4)[(i + k) % 3] for k in range(3)]
        held = [0]
        for k in range(step):
            held += [s ^ bits[k] for s in held]
        return held, bits[step]

    def all_spread(step):
        copies = []
        for i in range(3):
            held, bit = step_slots(i, step)
            for slot in held:
                for h in range(2):
                    copies.append(spread(h, i, slot, bit))
        return copies

    sub = lax.broadcasted_iota(jnp.int32, (16, TOK), 0) % 8
    before = lax.broadcasted_iota(jnp.int32, (TOK, TOK), 0)
    after = lax.broadcasted_iota(jnp.int32, (TOK, TOK), 1)
    earlier = jnp.where(before < after, 1.0, 0.0).astype(jnp.bfloat16)

    def group_row(h, g):
        return pick(g, SHARE[h](y), y), PAIR[h](z) * 2 + PAIR[h](x)

    def build(h, g):
        ys, block = group_row(h, g)
        names = [ids[h, ys * 4 + block, k] for k in range(8)]

        def marks(d, carry):
            owner = target(h, d)
            for e in range(2):
                hit = names[0] == owner * 2 + e
                for k in range(1, 8):
                    hit = hit | (names[k] == owner * 2 + e)
                mk[pl.ds(pl.multiple_of(d * 16 + e * 8, 8), 8), :] = jnp.where(hit, 1.0, 0.0)
            return carry

        lax.fori_loop(0, 16, marks, 0)
        marked = mk[...]
        rank = jnp.dot(marked.astype(jnp.bfloat16), earlier, preferred_element_type=jnp.float32)
        rk[...] = jnp.where(marked > 0.5, rank, -1.0)

        def places(d, carry):
            for e in range(2):
                rank_e = rk[pl.ds(pl.multiple_of(d * 16 + e * 8, 8), 8), :]
                for j in range(0, CAP, 2):
                    hit = jnp.concatenate(
                        [jnp.where(rank_e == float(j + q), 1.0, 0.0) for q in range(2)], axis=0
                    )
                    for k in range(8):
                        own = (
                            pick(k // 4, 1 - MEMBER[h](z), MEMBER[h](z)) * 4
                            + pick((k // 2) % 2, 1 - MEMBER[h](x), MEMBER[h](x)) * 2
                            + k % 2
                        )
                        oh[h, g, d, e * 48 + j * 8 : e * 48 + j * 8 + 16, k * TOK : (k + 1) * TOK] = (
                            jnp.where(sub == own, hit, 0.0).astype(jnp.bfloat16)
                        )
            return carry

        lax.fori_loop(0, 16, places, 0)

    for copy in loads:
        copy.wait()
    for copy in swaps:
        copy.wait_recv()
    first = all_spread(0)
    for copy in first:
        copy.start()
    build(0, 0)
    for copy in first:
        copy.wait_recv()
    second = all_spread(1)
    for copy in second:
        copy.start()
    build(1, 0)
    for copy in second:
        copy.wait_recv()
    third = all_spread(2)
    for copy in third:
        copy.start()
    build(0, 1)
    build(1, 1)
    for copy in third:
        copy.wait_recv()

    def put(h, u, d):
        g, n = u // 8, (u // 4) % 2
        ys, block = group_row(h, g)
        return (
            sb.at[h, u // 4, d],
            out.at[
                h,
                :,
                pl.ds(pl.multiple_of(ys * 192 + block * 48, 16), 48),
                pl.ds(pl.multiple_of(core * QUARTER + n * PIECE, 128), PIECE),
            ],
        )

    def remote(h, u, d):
        src, dst = put(h, u, d)
        return pltpu.make_async_remote_copy(
            src_ref=src,
            dst_ref=dst,
            send_sem=put_send.at[h, u // 4, d],
            recv_sem=put_recv.at[h, u // 4, d],
            device_id=(target(h, d),),
            device_id_type=MESH,
        )

    def local(h, u):
        src, dst = put(h, u, 0)
        return pltpu.make_async_copy(src, dst, keep_sem.at[h, u // 4])

    def send(h, u):
        for q in range(4):
            d = (u % 4) * 4 + q
            if q == 0:
                @pl.when(u % 4 == 0)
                def _():
                    local(h, u).start()

                @pl.when(u % 4 != 0)
                def _():
                    remote(h, u, d).start()
            else:
                remote(h, u, d).start()

    def pack(u, carry):
        g, n, m = u // 8, (u // 4) % 2, u % 4
        for h in range(2):
            placer = oh[h, g, pl.ds(m * 4, 4)].reshape(384, 1024)
            rows = xg[h, pl.ds(g * 4, 4), :, pl.ds(pl.multiple_of(n * PIECE, 128), PIECE)]
            packed = jnp.dot(placer, rows.reshape(1024, PIECE), preferred_element_type=jnp.float32)
            sb[h, u // 4, pl.ds(m * 4, 4)] = packed.astype(jnp.bfloat16).reshape(4, 2, 48, PIECE)

            @pl.when(u > 0)
            def _():
                send(h, u - 1)
        return carry

    lax.fori_loop(0, 16, pack, 0)
    for h in range(2):
        send(h, 15)

    for copy in first + second + third:
        copy.wait_send()
    for copy in swaps:
        copy.wait_send()

    def drain(w, carry):
        for h in range(2):
            local(h, w * 4).wait()

            def one(d, inner):
                remote(h, w * 4, d).wait()
                return inner

            lax.fori_loop(1, 16, one, 0)
        return carry

    lax.fori_loop(0, 4, drain, 0)


def place(goal, rows, out, placer):
    @pl.when(pl.program_id(2) == 0)
    def _():
        line = lax.broadcasted_iota(jnp.int32, (LINES, LINES), 0)
        placer[...] = jnp.where(goal[0, 0] == line, 1.0, 0.0).astype(jnp.bfloat16)

    out[0] = jnp.dot(placer[...], rows[0, 0], preferred_element_type=jnp.float32).astype(jnp.bfloat16)


def regroup(table, h):
    if ORDER[h] is not None:
        table = jnp.concatenate([table[:, i : i + 1] for i in ORDER[h]], axis=1)
        table = jnp.concatenate([table[:, :, i : i + 1] for i in ORDER[h]], axis=2)
    rest = table.shape[4:]
    table = table.reshape(4, 2, 2, 2, 2, 2, *rest)
    return jnp.transpose(table, (0, 1, 3, 2, 4, 5) + tuple(range(6, 6 + len(rest))))


def shards(tokens, expert_ids):
    me = lax.axis_index("ep")
    every = lax.all_gather(expert_ids.T, "ep")
    grid = every.reshape(4, 4, 4, 2, TOP, TOK)
    ids = jnp.stack(
        [
            jnp.transpose(regroup(grid, h).reshape(16, 8, TOP, TOK), (0, 2, 1, 3))
            for h in range(2)
        ]
    )
    mine = me * 2 + jnp.arange(2, dtype=jnp.int32)
    counts = jnp.sum((every[:, :, :, None] == mine).astype(jnp.int32), axis=(1, 2))
    index = jnp.arange(128, dtype=jnp.int32)
    offsets = jnp.sum(
        jnp.where(index[:, None, None] > index[None, :, None], counts[None], 0), axis=1
    )
    totals = jnp.sum(counts, axis=0)
    slot = jnp.arange(CAP, dtype=jnp.int32)[:, None]
    goals = []
    for h in range(2):
        have = regroup(counts.reshape(4, 4, 4, 2, 2), h).reshape(16, 1, 8, 2)
        start = regroup(offsets.reshape(4, 4, 4, 2, 2), h).reshape(16, 1, 8, 2)
        goal = jnp.where(slot[None, :, :, None] < have, start + slot[None, :, :, None], -1)
        goals.append(jnp.transpose(goal.reshape(LINES, 2)))
    goals = jnp.stack(goals).reshape(2, 2, 1, LINES)

    arrived = pl.pallas_call(
        exchange,
        out_shape=jax.ShapeDtypeStruct((2, 2, LINES, HALF), jnp.bfloat16),
        in_specs=[
            pl.BlockSpec(memory_space=pl.ANY),
            pl.BlockSpec(memory_space=pltpu.VMEM),
        ],
        out_specs=pl.BlockSpec(memory_space=pl.ANY),
        scratch_shapes=[
            pltpu.VMEM((2, 8, 2 * TOK, QUARTER), jnp.bfloat16),
            pltpu.VMEM((2, 2, 16, 96, 8 * TOK), jnp.bfloat16),
            pltpu.VMEM((2, 4, 16, 2, 48, PIECE), jnp.bfloat16),
            pltpu.VMEM((256, TOK), jnp.float32),
            pltpu.VMEM((256, TOK), jnp.float32),
            pltpu.SemaphoreType.DMA((2,)),
            pltpu.SemaphoreType.DMA((2,)),
            pltpu.SemaphoreType.DMA((2,)),
            pltpu.SemaphoreType.DMA((2, 3, 8)),
            pltpu.SemaphoreType.DMA((2, 3, 8)),
            pltpu.SemaphoreType.DMA((2, 4, 16)),
            pltpu.SemaphoreType.DMA((2, 4, 16)),
            pltpu.SemaphoreType.DMA((2, 4)),
        ],
        compiler_params=pltpu.CompilerParams(
            collective_id=0, has_side_effects=True, vmem_limit_bytes=62 * 1024 * 1024
        ),
        name="exchange",
    )(tokens, ids)

    merged = pl.pallas_call(
        place,
        out_shape=jax.ShapeDtypeStruct((2, LINES, WIDTH), jnp.bfloat16),
        grid=(2, 2, 4),
        in_specs=[
            pl.BlockSpec((1, 1, 1, LINES), lambda e, h, n: (h, e, 0, 0)),
            pl.BlockSpec((1, 1, LINES, HALF // 4), lambda e, h, n: (h, e, 0, n)),
        ],
        out_specs=pl.BlockSpec((1, LINES, HALF // 4), lambda e, h, n: (e, 0, h * 4 + n)),
        scratch_shapes=[pltpu.VMEM((LINES, LINES), jnp.bfloat16)],
        name="place",
    )(goals, arrived)
    return (merged, totals)


def solution(mesh):
    in_specs = (P("ep", None), P("ep", None))
    out_specs = (P("ep", None, None), P("ep"))
    return jax.shard_map(shards, mesh=mesh, in_specs=in_specs, out_specs=out_specs, check_vma=False)
```

```python
import functools

import jax
import jax.numpy as jnp
from jax import lax
from jax.experimental import pallas as pl
from jax.experimental.pallas import tpu as pltpu
from jax.sharding import PartitionSpec as P

EXPERTS = 256
CAP = 6
TOP = 8
TOK = 128
WIDTH = 7168
HALF = WIDTH // 2
QUARTER = HALF // 2
PIECE = QUARTER // 2
LINES = 768
SPLITS = (((0, 384), (384, 256), (640, 256)), ((896, 256), (1152, 384), (1536, 256)))
MESH = pl.DeviceIdType.MESH
WINDOW = 208


def near(v):
    return v + 1 - 2 * (v % 2)


def far(v):
    return 3 - v


SHARE = (near, far)
CROSS = (far, near)
PAIR = (lambda v: v // 2, lambda v: ((v + 1) // 2) % 2)
MEMBER = (lambda v: v % 2, lambda v: v // 2)
SPOT = (lambda p, m: p * 2 + m, lambda p, m: p + m * (3 - 2 * p))


def pick(flag, flipped, value):
    return value + flag * (flipped - value)


def exchange(tok, ids, out, goal, starts, xg, oh, sb, mk, rk, idr, cts, ctr,
             load_sem, swap_send, swap_recv, id_sem, id_send, id_recv, ag_send, ag_recv,
             count_send, count_recv, put_send, put_recv, keep_sem):
    me = lax.axis_index("ep")
    core, x, z, y = me % 2, (me // 2) % 4, (me // 8) % 4, me // 32

    def device(yy, zz, xx, cc):
        return ((yy * 4 + zz) * 4 + xx) * 2 + cc

    def target(flip, d):
        return device(
            pick(d // 8, flip(y), y),
            pick((d // 4) % 2, flip(z), z),
            pick((d // 2) % 2, flip(x), x),
            pick(d % 2, 1 - core, core),
        )

    loads = []
    for h in range(2):
        loads.append(
            pltpu.make_async_copy(
                tok.at[:, pl.ds(pl.multiple_of(h * HALF + core * QUARTER, 128), QUARTER)],
                xg.at[h, 0, pl.ds(pl.multiple_of(core * TOK, TOK), TOK), :],
                load_sem.at[h],
            )
        )
        loads.append(pltpu.make_async_copy(ids, idr.at[h, 0], id_sem.at[h]))
    for copy in loads:
        copy.start()

    barrier = pltpu.get_barrier_semaphore()
    for h in range(2):
        for d in range(1, 16):
            if h == 0 or d >= 2:
                pl.semaphore_signal(
                    barrier, inc=1, device_id=(target(CROSS[h], d),), device_id_type=MESH
                )
    pl.semaphore_wait(barrier, 29)

    partner = device(y, z, x, 1 - core)
    swaps = []
    for h in range(2):
        copy = pltpu.make_async_remote_copy(
            src_ref=tok.at[:, pl.ds(pl.multiple_of(h * HALF + (1 - core) * QUARTER, 128), QUARTER)],
            dst_ref=xg.at[h, 0, pl.ds(pl.multiple_of(core * TOK, TOK), TOK), :],
            send_sem=swap_send.at[h],
            recv_sem=swap_recv.at[h],
            device_id=(partner,),
            device_id_type=MESH,
        )
        copy.start()
        swaps.append(copy)
    names_sent = []
    for d in range(1, 16):
        for h in range(2):
            copy = pltpu.make_async_remote_copy(
                src_ref=ids,
                dst_ref=idr.at[h, d],
                send_sem=id_send.at[h, d],
                recv_sem=id_recv.at[h, d],
                device_id=(target(SHARE[h], d),),
                device_id_type=MESH,
            )
            copy.start()
            names_sent.append(copy)

    def neighbour(h, bit):
        flip = SHARE[h]
        if bit == 1:
            return device(y, z, flip(x), core)
        if bit == 2:
            return device(y, flip(z), x, core)
        return device(flip(y), z, x, core)

    def spread(h, n, i, slot, bit):
        at, size = SPLITS[n][i]
        return pltpu.make_async_remote_copy(
            src_ref=xg.at[h, slot, :, pl.ds(at, size)],
            dst_ref=xg.at[h, slot ^ bit, :, pl.ds(at, size)],
            send_sem=ag_send.at[h, n, i, slot ^ bit],
            recv_sem=ag_recv.at[h, n, i, slot ^ bit],
            device_id=(neighbour(h, bit),),
            device_id_type=MESH,
        )

    def spread_step(n, step):
        copies = []
        for i in range(3):
            bits = [(1, 2, 4)[(i + k) % 3] for k in range(3)]
            held = [0]
            for k in range(step):
                held += [s ^ bits[k] for s in held]
            for slot in held:
                for h in range(2):
                    copies.append(spread(h, n, i, slot, bits[step]))
        return copies

    sub = lax.broadcasted_iota(jnp.int32, (16, TOK), 0) % 8
    lane = lax.broadcasted_iota(jnp.int32, (8, TOK), 1)
    before = lax.broadcasted_iota(jnp.int32, (TOK, TOK), 0)
    after = lax.broadcasted_iota(jnp.int32, (TOK, TOK), 1)
    earlier = jnp.where(before < after, 1.0, 0.0).astype(jnp.bfloat16)
    ones = jnp.ones((TOK, TOK), jnp.bfloat16)

    def group_row(h, g):
        return pick(g, SHARE[h](y), y), PAIR[h](z) * 2 + PAIR[h](x)

    def source_place(h, k):
        return (
            pick(k // 4, 1 - MEMBER[h](z), MEMBER[h](z)) * 4
            + pick((k // 2) % 2, 1 - MEMBER[h](x), MEMBER[h](x)) * 2
            + k % 2
        )

    def build(h, g):
        slots = [(g * 4 + k // 2) * 2 + pick(k % 2, 1 - core, core) for k in range(8)]
        names = []
        for q in range(TOP):
            rows = jnp.zeros((8, TOK), jnp.int32)
            for k in range(8):
                rows = jnp.where(sub[:8] == source_place(h, k), idr[h, slots[k], q : q + 1, :], rows)
            names.append(rows)

        def marks(d, carry):
            owner = target(CROSS[h], d)
            for e in range(2):
                hit = names[0] == owner * 2 + e
                for q in range(1, TOP):
                    hit = hit | (names[q] == owner * 2 + e)
                mk[pl.ds(pl.multiple_of(d * 16 + e * 8, 8), 8), :] = jnp.where(hit, 1.0, 0.0)
            return carry

        lax.fori_loop(0, 16, marks, 0)
        marked = mk[...]
        whole = marked.astype(jnp.bfloat16)
        rank = jnp.dot(whole, earlier, preferred_element_type=jnp.float32)
        rk[...] = jnp.where(marked > 0.5, rank, -1.0)
        if h == 0:
            mk[...] = jnp.dot(whole, ones, preferred_element_type=jnp.float32)
            member = pick(g, 1 - y % 2, y % 2)
            for flips in range(8):
                tile = cts[flips]
                for e in range(2):
                    tile = jnp.where(
                        lane // 32 == member * 2 + e,
                        mk[flips * 32 + e * 8 : flips * 32 + e * 8 + 8, :],
                        tile,
                    )
                cts[flips] = tile

        def places(d, carry):
            for e in range(2):
                rank_e = rk[pl.ds(pl.multiple_of(d * 16 + e * 8, 8), 8), :]
                for j in range(0, CAP, 2):
                    hit = jnp.concatenate(
                        [jnp.where(rank_e == float(j + q), 1.0, 0.0) for q in range(2)], axis=0
                    )
                    for k in range(8):
                        oh[h, g, d, e * 48 + j * 8 : e * 48 + j * 8 + 16, k * TOK : (k + 1) * TOK] = (
                            jnp.where(sub == source_place(h, k), hit, 0.0).astype(jnp.bfloat16)
                        )
            return carry

        lax.fori_loop(0, 16, places, 0)

    cts[...] = jnp.zeros(cts.shape, jnp.float32)
    for copy in loads:
        copy.wait()
    for copy in swaps:
        copy.wait_recv()
    first = [spread_step(n, 0) for n in range(2)]
    for n in range(2):
        for copy in first[n]:
            copy.start()
    for copy in names_sent:
        copy.wait_recv()
    build(0, 0)
    second = [spread_step(n, 1) for n in range(2)]
    for n in range(2):
        for copy in first[n]:
            copy.wait_recv()
        for copy in second[n]:
            copy.start()
    build(0, 1)
    third = [spread_step(n, 2) for n in range(2)]
    for n in range(2):
        for copy in second[n]:
            copy.wait_recv()
        for copy in third[n]:
            copy.start()

    block = (y // 2) * 4 + (z // 2) * 2 + x // 2
    counts = []
    for flips in range(1, 8):
        copy = pltpu.make_async_remote_copy(
            src_ref=cts.at[flips],
            dst_ref=ctr.at[block],
            send_sem=count_send.at[flips],
            recv_sem=count_recv.at[flips],
            device_id=(target(far, flips * 2),),
            device_id_type=MESH,
        )
        copy.start()
        counts.append(copy)
    own_count = pltpu.make_async_copy(cts.at[0], ctr.at[block], count_send.at[0])
    own_count.start()
    build(1, 0)
    build(1, 1)

    def put(h, n, w, d):
        ys, where = group_row(h, w // 4)
        return (
            sb.at[h, n, w // 4, d],
            out.at[
                h,
                :,
                pl.ds(pl.multiple_of(ys * 192 + where * 48, 16), 48),
                pl.ds(pl.multiple_of(core * QUARTER + n * PIECE, 128), PIECE),
            ],
        )

    def remote(h, n, w, d):
        src, dst = put(h, n, w, d)
        return pltpu.make_async_remote_copy(
            src_ref=src,
            dst_ref=dst,
            send_sem=put_send.at[h, n, w // 4, d],
            recv_sem=put_recv.at[h, n, w // 4, d],
            device_id=(target(CROSS[h], d),),
            device_id_type=MESH,
        )

    def local(h, n, w):
        src, dst = put(h, n, w, 0)
        return pltpu.make_async_copy(src, dst, keep_sem.at[h, n, w // 4])

    def send(h, n, w):
        for q in range(3, -1, -1):
            d = (3 - w % 4) * 4 + q
            if q == 0:
                @pl.when(w % 4 == 3)
                def _():
                    local(h, n, w).start()

                @pl.when(w % 4 != 3)
                def _():
                    remote(h, n, w, d).start()
            else:
                remote(h, n, w, d).start()

    for n in range(2):
        for copy in third[n]:
            copy.wait_recv()

        def pack(w, carry, n=n):
            g, m = w // 4, 3 - w % 4
            for h in range(2):
                placer = oh[h, g, pl.ds(m * 4, 4)].reshape(384, 1024)
                rows = xg[h, pl.ds(g * 4, 4), :, n * PIECE : (n + 1) * PIECE]
                packed = jnp.dot(
                    placer, rows.reshape(1024, PIECE), preferred_element_type=jnp.float32
                )
                sb[h, n, g, pl.ds(m * 4, 4)] = packed.astype(jnp.bfloat16).reshape(4, 2, 48, PIECE)

                @pl.when(w > 0)
                def _():
                    send(h, n, w - 1)
            return carry

        lax.fori_loop(0, 8, pack, 0)
        for h in range(2):
            send(h, n, 7)

    own_count.wait()
    for copy in counts:
        copy.wait_recv()
    table = ctr[...].reshape(64, TOK).astype(jnp.bfloat16)
    row = lax.broadcasted_iota(jnp.int32, (64, 192), 0)
    col = lax.broadcasted_iota(jnp.int32, (64, 192), 1)
    row_z = SPOT[0]((row // 16) % 2, (row // 4) % 2)
    row_x = SPOT[0]((row // 8) % 2, (row // 2) % 2)
    turn = (((0,), (0,)), ((), ()))
    slot = (lax.broadcasted_iota(jnp.int32, (1, 192), 1) % 48) // 8
    for h in range(2):
        col_z = SPOT[h](col // 96, (col % 8) // 4)
        col_x = SPOT[h]((col // 48) % 2, (col // 2) % 2)
        for yy in range(4):
            there = device(yy, col_z, col_x, col % 2)
            base = [jnp.zeros((1, 192), jnp.float32) for _ in range(2)]
            have = [jnp.zeros((1, 192), jnp.float32) for _ in range(2)]
            for member in range(2):
                here = device((row // 32) * 2 + member, row_z, row_x, row % 2)
                below = jnp.where(here < there, 1.0, 0.0).astype(jnp.bfloat16)
                same = jnp.where(here == there, 1.0, 0.0).astype(jnp.bfloat16)
                below = lax.dot_general(table, below, turn, preferred_element_type=jnp.float32)
                same = lax.dot_general(table, same, turn, preferred_element_type=jnp.float32)
                for e in range(2):
                    at = member * 64 + e * 32
                    base[e] = base[e] + below[at : at + 1, :]
                    have[e] = have[e] + same[at : at + 1, :]
            for e in range(2):
                at = base[e].astype(jnp.int32)
                mine = (h * 2 + e) * 4 + yy
                goal[mine : mine + 1, 0:192] = jnp.where(slot < have[e].astype(jnp.int32), at + slot, -1)
                if h == 0:
                    starts[e * 4 + yy : e * 4 + yy + 1, :] = at[:, 0:TOK]
    sums = lax.dot_general(
        table, jnp.ones((64, TOK), jnp.bfloat16), turn, preferred_element_type=jnp.float32
    )
    for e in range(2):
        starts[8 + e : 9 + e, :] = (
            sums[e * 32 : e * 32 + 1, :] + sums[64 + e * 32 : 65 + e * 32, :]
        ).astype(jnp.int32)

    for copy in names_sent + counts + swaps:
        copy.wait_send()
    for step in (first, second, third):
        for n in range(2):
            for copy in step[n]:
                copy.wait_send()

    for n in range(2):

        def drain(g, carry, n=n):
            for h in range(2):
                local(h, n, g * 4).wait()

                def one(d, inner, h=h):
                    remote(h, n, g * 4, d).wait()
                    return inner

                lax.fori_loop(1, 16, one, 0)
            return carry

        lax.fori_loop(0, 2, drain, 0)


def place(starts, goal, rows, out, totals, placer):
    e, h, n = pl.program_id(0), pl.program_id(1), pl.program_id(2)

    def window(yy):
        return pl.multiple_of(jnp.minimum(starts[e * 4 + yy, 0] // 16 * 16, LINES - WINDOW), 16)

    @pl.when(n == 0)
    def _():
        totals[e] = starts[8 + e, 0]
        line = lax.broadcasted_iota(jnp.int32, (WINDOW, 192), 0)
        for yy in range(4):
            wanted = goal[pl.ds((h * 2 + e) * 4 + yy, 1), 0:192] - window(yy)
            placer[yy] = jnp.where(wanted == line, 1.0, 0.0).astype(jnp.bfloat16)

    out[...] = jnp.zeros(out.shape, jnp.bfloat16)
    for yy in range(4):
        part = jnp.dot(
            placer[yy], rows[0, 0, yy * 192 : (yy + 1) * 192, :], preferred_element_type=jnp.float32
        ).astype(jnp.bfloat16)
        span = pl.ds(window(yy), WINDOW)
        out[0, span, :] = out[0, span, :] + part


def shards(tokens, expert_ids):
    anywhere = pl.BlockSpec(memory_space=pl.ANY)
    vmem = pl.BlockSpec(memory_space=pltpu.VMEM)
    arrived, goal, starts = pl.pallas_call(
        exchange,
        out_shape=(
            jax.ShapeDtypeStruct((2, 2, LINES, HALF), jnp.bfloat16),
            jax.ShapeDtypeStruct((16, 256), jnp.int32),
            jax.ShapeDtypeStruct((16, TOK), jnp.int32),
        ),
        in_specs=[anywhere, vmem],
        out_specs=(anywhere, vmem, vmem),
        scratch_shapes=[
            pltpu.VMEM((2, 8, 2 * TOK, QUARTER), jnp.bfloat16),
            pltpu.VMEM((2, 2, 16, 96, 8 * TOK), jnp.bfloat16),
            pltpu.VMEM((2, 2, 2, 16, 2, 48, PIECE), jnp.bfloat16),
            pltpu.VMEM((256, TOK), jnp.float32),
            pltpu.VMEM((256, TOK), jnp.float32),
            pltpu.VMEM((2, 16, TOP, TOK), jnp.int32),
            pltpu.VMEM((8, 8, TOK), jnp.float32),
            pltpu.VMEM((8, 8, TOK), jnp.float32),
            pltpu.SemaphoreType.DMA((2,)),
            pltpu.SemaphoreType.DMA((2,)),
            pltpu.SemaphoreType.DMA((2,)),
            pltpu.SemaphoreType.DMA((2,)),
            pltpu.SemaphoreType.DMA((2, 16)),
            pltpu.SemaphoreType.DMA((2, 16)),
            pltpu.SemaphoreType.DMA((2, 2, 3, 8)),
            pltpu.SemaphoreType.DMA((2, 2, 3, 8)),
            pltpu.SemaphoreType.DMA((8,)),
            pltpu.SemaphoreType.DMA((8,)),
            pltpu.SemaphoreType.DMA((2, 2, 2, 16)),
            pltpu.SemaphoreType.DMA((2, 2, 2, 16)),
            pltpu.SemaphoreType.DMA((2, 2, 2)),
        ],
        compiler_params=pltpu.CompilerParams(
            collective_id=0, has_side_effects=True, vmem_limit_bytes=62 * 1024 * 1024
        ),
        name="exchange",
    )(tokens, expert_ids.T)

    return pl.pallas_call(
        place,
        out_shape=(
            jax.ShapeDtypeStruct((2, LINES, WIDTH), jnp.bfloat16),
            jax.ShapeDtypeStruct((2,), jnp.int32),
        ),
        grid=(2, 2, 4),
        in_specs=[
            pl.BlockSpec(memory_space=pltpu.SMEM),
            vmem,
            pl.BlockSpec((1, 1, LINES, HALF // 4), lambda e, h, n: (h, e, 0, n)),
        ],
        out_specs=(
            pl.BlockSpec((1, LINES, HALF // 4), lambda e, h, n: (e, 0, h * 4 + n)),
            pl.BlockSpec(memory_space=pltpu.SMEM),
        ),
        scratch_shapes=[pltpu.VMEM((4, WINDOW, 192), jnp.bfloat16)],
        name="place",
    )(starts, goal, arrived)


def solution(mesh):
    in_specs = (P("ep", None), P("ep", None))
    out_specs = (P("ep", None, None), P("ep"))
    return jax.shard_map(shards, mesh=mesh, in_specs=in_specs, out_specs=out_specs, check_vma=False)
```

```python
import functools

import jax
import jax.numpy as jnp
from jax import lax
from jax.experimental import pallas as pl
from jax.experimental.pallas import tpu as pltpu
from jax.sharding import PartitionSpec as P

EXPERTS = 256
CAP = 6
TOP = 8
TOK = 128
WIDTH = 7168
HALF = WIDTH // 2
QUARTER = HALF // 2
PIECE = QUARTER // 2
LINES = 768
SPLITS = (((0, 384), (384, 256), (640, 256)), ((896, 256), (1152, 384), (1536, 256)))
MESH = pl.DeviceIdType.MESH
WINDOW = 208


def near(v):
    return v + 1 - 2 * (v % 2)


def far(v):
    return 3 - v


SHARE = (near, far)
CROSS = (far, near)
PAIR = (lambda v: v // 2, lambda v: ((v + 1) // 2) % 2)
MEMBER = (lambda v: v % 2, lambda v: v // 2)
SPOT = (lambda p, m: p * 2 + m, lambda p, m: p + m * (3 - 2 * p))


def pick(flag, flipped, value):
    return value + flag * (flipped - value)


def exchange(tok, ids, out, goal, starts, xg, oh, sb, via, onward, mk, rk, idr, cts, ctr,
             load_sem, swap_send, swap_recv, id_sem, id_send, id_recv, own_send, own_recv,
             ag_send, ag_recv, count_send, count_recv, via_send, via_recv, onward_send,
             onward_recv, put_send, put_recv, keep_sem):
    me = lax.axis_index("ep")
    core, x, z, y = me % 2, (me // 2) % 4, (me // 8) % 4, me // 32

    def device(yy, zz, xx, cc):
        return ((yy * 4 + zz) * 4 + xx) * 2 + cc

    def target(flip, d):
        return device(
            pick(d // 8, flip(y), y),
            pick((d // 4) % 2, flip(z), z),
            pick((d // 2) % 2, flip(x), x),
            pick(d % 2, 1 - core, core),
        )

    loads = []
    for h in range(2):
        loads.append(
            pltpu.make_async_copy(
                tok.at[:, pl.ds(pl.multiple_of(h * HALF + core * QUARTER, 128), QUARTER)],
                xg.at[h, 0, pl.ds(pl.multiple_of(core * TOK, TOK), TOK), :],
                load_sem.at[h],
            )
        )
        loads.append(pltpu.make_async_copy(ids, idr.at[h, 0], id_sem.at[h]))
    for copy in loads:
        copy.start()

    barrier = pltpu.get_barrier_semaphore()
    for h in range(2):
        for d in range(1, 16):
            if h == 0 or d >= 2:
                pl.semaphore_signal(
                    barrier, inc=1, device_id=(target(CROSS[h], d),), device_id_type=MESH
                )
    pl.semaphore_wait(barrier, 29)

    partner = device(y, z, x, 1 - core)
    swaps = []
    for h in range(2):
        copy = pltpu.make_async_remote_copy(
            src_ref=tok.at[:, pl.ds(pl.multiple_of(h * HALF + (1 - core) * QUARTER, 128), QUARTER)],
            dst_ref=xg.at[h, 0, pl.ds(pl.multiple_of(core * TOK, TOK), TOK), :],
            send_sem=swap_send.at[h],
            recv_sem=swap_recv.at[h],
            device_id=(partner,),
            device_id_type=MESH,
        )
        copy.start()
        swaps.append(copy)
    def neighbour(h, bit):
        flip = SHARE[h]
        if bit == 1:
            return device(y, z, flip(x), core)
        if bit == 2:
            return device(y, flip(z), x, core)
        return device(flip(y), z, x, core)

    def spread(h, n, i, slot, bit):
        at, size = SPLITS[n][i]
        return pltpu.make_async_remote_copy(
            src_ref=xg.at[h, slot, :, pl.ds(at, size)],
            dst_ref=xg.at[h, slot ^ bit, :, pl.ds(at, size)],
            send_sem=ag_send.at[h, n, i, slot ^ bit],
            recv_sem=ag_recv.at[h, n, i, slot ^ bit],
            device_id=(neighbour(h, bit),),
            device_id_type=MESH,
        )

    def spread_own(h, n, i, other):
        at, size = SPLITS[n][i]
        cc = 1 - core if other else core
        bit = (1, 2, 4)[i]
        return pltpu.make_async_remote_copy(
            src_ref=tok.at[:, pl.ds(pl.multiple_of(h * HALF + cc * QUARTER + at, 128), size)],
            dst_ref=xg.at[h, bit, pl.ds(pl.multiple_of(core * TOK, TOK), TOK), pl.ds(at, size)],
            send_sem=own_send.at[h, n, i, other],
            recv_sem=own_recv.at[h, n, i, other],
            device_id=(neighbour(h, bit) + cc - core,),
            device_id_type=MESH,
        )

    def spread_step(n, step):
        copies = []
        for i in range(3):
            bits = [(1, 2, 4)[(i + k) % 3] for k in range(3)]
            held = [0]
            for k in range(step):
                held += [s ^ bits[k] for s in held]
            for slot in held:
                for h in range(2):
                    if step == 0:
                        copies += [spread_own(h, n, i, other) for other in range(2)]
                    else:
                        copies.append(spread(h, n, i, slot, bits[step]))
        return copies

    sub = lax.broadcasted_iota(jnp.int32, (16, TOK), 0) % 8
    lane = lax.broadcasted_iota(jnp.int32, (8, TOK), 1)
    before = lax.broadcasted_iota(jnp.int32, (TOK, TOK), 0)
    after = lax.broadcasted_iota(jnp.int32, (TOK, TOK), 1)
    earlier = jnp.where(before < after, 1.0, 0.0).astype(jnp.bfloat16)
    ones = jnp.ones((TOK, TOK), jnp.bfloat16)

    def group_row(h, g):
        return pick(g, SHARE[h](y), y), PAIR[h](z) * 2 + PAIR[h](x)

    def source_place(h, k):
        return (
            pick(k // 4, 1 - MEMBER[h](z), MEMBER[h](z)) * 4
            + pick((k // 2) % 2, 1 - MEMBER[h](x), MEMBER[h](x)) * 2
            + k % 2
        )

    def build(h, g):
        slots = [(g * 4 + k // 2) * 2 + pick(k % 2, 1 - core, core) for k in range(8)]
        names = []
        for q in range(TOP):
            rows = jnp.zeros((8, TOK), jnp.int32)
            for k in range(8):
                rows = jnp.where(sub[:8] == source_place(h, k), idr[h, slots[k], q : q + 1, :], rows)
            names.append(rows)

        def marks(d, carry):
            owner = target(CROSS[h], d)
            for e in range(2):
                hit = names[0] == owner * 2 + e
                for q in range(1, TOP):
                    hit = hit | (names[q] == owner * 2 + e)
                mk[pl.ds(pl.multiple_of(d * 16 + e * 8, 8), 8), :] = jnp.where(hit, 1.0, 0.0)
            return carry

        lax.fori_loop(0, 16, marks, 0)
        marked = mk[...]
        whole = marked.astype(jnp.bfloat16)
        rank = jnp.dot(whole, earlier, preferred_element_type=jnp.float32)
        rk[...] = jnp.where(marked > 0.5, rank, -1.0)
        if h == 0:
            mk[...] = jnp.dot(whole, ones, preferred_element_type=jnp.float32)
            member = pick(g, 1 - y % 2, y % 2)
            for flips in range(8):
                tile = cts[flips]
                for e in range(2):
                    tile = jnp.where(
                        lane // 32 == member * 2 + e,
                        mk[flips * 32 + e * 8 : flips * 32 + e * 8 + 8, :],
                        tile,
                    )
                cts[flips] = tile

        def places(d, carry):
            for e in range(2):
                rank_e = rk[pl.ds(pl.multiple_of(d * 16 + e * 8, 8), 8), :]
                for j in range(0, CAP, 2):
                    hit = jnp.concatenate(
                        [jnp.where(rank_e == float(j + q), 1.0, 0.0) for q in range(2)], axis=0
                    )
                    for k in range(8):
                        oh[h, g, d, e * 48 + j * 8 : e * 48 + j * 8 + 16, k * TOK : (k + 1) * TOK] = (
                            jnp.where(sub == source_place(h, k), hit, 0.0).astype(jnp.bfloat16)
                        )
            return carry

        lax.fori_loop(0, 16, places, 0)

    first = [spread_step(n, 0) for n in range(2)]
    for copy in first[0]:
        copy.start()
    names_sent = []
    for d in range(1, 16):
        for h in range(2):
            copy = pltpu.make_async_remote_copy(
                src_ref=ids,
                dst_ref=idr.at[h, d],
                send_sem=id_send.at[h, d],
                recv_sem=id_recv.at[h, d],
                device_id=(target(SHARE[h], d),),
                device_id_type=MESH,
            )
            copy.start()
            names_sent.append(copy)

    for copy in first[1]:
        copy.start()
    cts[...] = jnp.zeros(cts.shape, jnp.float32)
    for copy in loads:
        copy.wait()
    for copy in swaps:
        copy.wait_recv()
    for copy in names_sent:
        copy.wait_recv()
    build(0, 0)
    second = [spread_step(n, 1) for n in range(2)]
    for n in range(2):
        for copy in first[n]:
            copy.wait_recv()
        for copy in second[n]:
            copy.start()
    build(0, 1)
    third = [spread_step(n, 2) for n in range(2)]
    for n in range(2):
        for copy in second[n]:
            copy.wait_recv()
        for copy in third[n]:
            copy.start()

    block = (y // 2) * 4 + (z // 2) * 2 + x // 2
    counts = []
    for flips in range(1, 8):
        copy = pltpu.make_async_remote_copy(
            src_ref=cts.at[flips],
            dst_ref=ctr.at[block],
            send_sem=count_send.at[flips],
            recv_sem=count_recv.at[flips],
            device_id=(target(far, flips * 2),),
            device_id_type=MESH,
        )
        copy.start()
        counts.append(copy)
    own_count = pltpu.make_async_copy(cts.at[0], ctr.at[block], count_send.at[0])
    own_count.start()
    build(1, 0)
    build(1, 1)

    def shift(h, bits):
        flip = CROSS[h]
        return (
            flip(y) if bits & 4 else y,
            flip(z) if bits & 2 else z,
            flip(x) if bits & 1 else x,
        )

    def landing(h, n, g, done):
        yy, zz, xx = shift(h, done)
        ys = SHARE[h](yy) if g else yy
        where = PAIR[h](zz) * 2 + PAIR[h](xx)
        return out.at[
            h,
            :,
            pl.ds(pl.multiple_of(ys * 192 + where * 48, 16), 48),
            pl.ds(pl.multiple_of(core * QUARTER + n * PIECE, 128), PIECE),
        ]

    def route(n, g):
        return [(1, 2, 4)[(n * 2 + g + k) % 3] for k in range(3)]

    def last_hop(h, n, g, cross, other):
        a, b, c = route(n, g)
        chunk = n * 2 + g
        bit = {a: a, b: b, a | b: b}.get(cross, 0 if cross == 0 else c)
        done = cross ^ bit
        if done == 0:
            src = sb.at[h, n, g, cross * 2 + other]
        elif done == a:
            src = via.at[h, chunk, 0 if cross == a | b else 1, other]
        else:
            src = onward.at[h, chunk, 0 if done == b else 1, other]
        return pltpu.make_async_remote_copy(
            src_ref=src,
            dst_ref=landing(h, n, g, done),
            send_sem=put_send.at[h, chunk, cross * 2 + other],
            recv_sem=put_recv.at[h, chunk, cross * 2 + other],
            device_id=(device(*shift(h, bit), 1 - core if other else core),),
            device_id_type=MESH,
        )

    def first_hop(h, n, g, which):
        a, b, c = route(n, g)
        cross = (a | b, a | c, a | b | c)[which]
        return pltpu.make_async_remote_copy(
            src_ref=sb.at[h, n, g, pl.ds(cross * 2, 2)],
            dst_ref=via.at[h, n * 2 + g, which],
            send_sem=via_send.at[h, n * 2 + g, which],
            recv_sem=via_recv.at[h, n * 2 + g, which],
            device_id=(device(*shift(h, a), core),),
            device_id_type=MESH,
        )

    def next_hop(h, n, g, which):
        a, b, c = route(n, g)
        chunk = n * 2 + g
        return pltpu.make_async_remote_copy(
            src_ref=sb.at[h, n, g, pl.ds((b | c) * 2, 2)] if which == 0 else via.at[h, chunk, 2],
            dst_ref=onward.at[h, chunk, which],
            send_sem=onward_send.at[h, chunk, which],
            recv_sem=onward_recv.at[h, chunk, which],
            device_id=(device(*shift(h, b), core),),
            device_id_type=MESH,
        )

    def keep(h, n, g):
        return pltpu.make_async_copy(
            sb.at[h, n, g, 0], landing(h, n, g, 0), keep_sem.at[h, n * 2 + g]
        )

    def pack(h, n, g):
        def some(m, carry):
            placer = oh[h, g, pl.ds(m * 4, 4)].reshape(384, 1024)
            rows = xg[h, g * 4 : g * 4 + 4, :, n * PIECE : (n + 1) * PIECE]
            packed = jnp.dot(placer, rows.reshape(1024, PIECE), preferred_element_type=jnp.float32)
            sb[h, n, g, pl.ds(m * 4, 4)] = packed.astype(jnp.bfloat16).reshape(4, 2, 48, PIECE)
            return carry

        lax.fori_loop(0, 4, some, 0)

    def leave(h, n, g):
        for which in (2, 0, 1):
            first_hop(h, n, g, which).start()
        next_hop(h, n, g, 0).start()
        keep(h, n, g).start()
        last_hop(h, n, g, 0, 1).start()

    def relay(h, n, g):
        a, b, c = route(n, g)
        first_hop(h, n, g, 2).wait_recv()
        next_hop(h, n, g, 1).start()
        for which, cross in ((0, a | b), (1, a | c)):
            first_hop(h, n, g, which).wait_recv()
            for other in range(2):
                last_hop(h, n, g, cross, other).start()
        for cross in (a, b, c):
            for other in range(2):
                last_hop(h, n, g, cross, other).start()

    def finish(h, n, g):
        a, b, c = route(n, g)
        for which, cross in ((0, b | c), (1, a | b | c)):
            next_hop(h, n, g, which).wait_recv()
            for other in range(2):
                last_hop(h, n, g, cross, other).start()

    units = [(h, n, g) for n in range(2) for g in range(2) for h in range(2)]
    for i, (h, n, g) in enumerate(units):
        if i % 4 == 0:
            for copy in third[n]:
                copy.wait_recv()
        pack(h, n, g)
        if i > 0:
            leave(*units[i - 1])
    relay(*units[0])
    leave(*units[-1])
    for unit in units[1:]:
        relay(*unit)

    own_count.wait()
    for copy in counts:
        copy.wait_recv()
    table = ctr[...].reshape(64, TOK).astype(jnp.bfloat16)
    row = lax.broadcasted_iota(jnp.int32, (64, 192), 0)
    col = lax.broadcasted_iota(jnp.int32, (64, 192), 1)
    row_z = SPOT[0]((row // 16) % 2, (row // 4) % 2)
    row_x = SPOT[0]((row // 8) % 2, (row // 2) % 2)
    turn = (((0,), (0,)), ((), ()))
    slot = (lax.broadcasted_iota(jnp.int32, (1, 192), 1) % 48) // 8
    for h in range(2):
        col_z = SPOT[h](col // 96, (col % 8) // 4)
        col_x = SPOT[h]((col // 48) % 2, (col // 2) % 2)
        for yy in range(4):
            there = device(yy, col_z, col_x, col % 2)
            base = [jnp.zeros((1, 192), jnp.float32) for _ in range(2)]
            have = [jnp.zeros((1, 192), jnp.float32) for _ in range(2)]
            for member in range(2):
                here = device((row // 32) * 2 + member, row_z, row_x, row % 2)
                below = jnp.where(here < there, 1.0, 0.0).astype(jnp.bfloat16)
                same = jnp.where(here == there, 1.0, 0.0).astype(jnp.bfloat16)
                below = lax.dot_general(table, below, turn, preferred_element_type=jnp.float32)
                same = lax.dot_general(table, same, turn, preferred_element_type=jnp.float32)
                for e in range(2):
                    at = member * 64 + e * 32
                    base[e] = base[e] + below[at : at + 1, :]
                    have[e] = have[e] + same[at : at + 1, :]
            for e in range(2):
                at = base[e].astype(jnp.int32)
                mine = (h * 2 + e) * 4 + yy
                goal[mine : mine + 1, 0:192] = jnp.where(slot < have[e].astype(jnp.int32), at + slot, -1)
                if h == 0:
                    starts[e * 4 + yy : e * 4 + yy + 1, :] = at[:, 0:TOK]
    sums = lax.dot_general(
        table, jnp.ones((64, TOK), jnp.bfloat16), turn, preferred_element_type=jnp.float32
    )
    for e in range(2):
        starts[8 + e : 9 + e, :] = (
            sums[e * 32 : e * 32 + 1, :] + sums[64 + e * 32 : 65 + e * 32, :]
        ).astype(jnp.int32)

    for unit in units:
        finish(*unit)

    for copy in names_sent + counts + swaps:
        copy.wait_send()
    for step in (first, second, third):
        for n in range(2):
            for copy in step[n]:
                copy.wait_send()
    for unit in units:
        for which in range(3):
            first_hop(*unit, which).wait_send()
        for which in range(2):
            next_hop(*unit, which).wait_send()
        keep(*unit).wait()
        for cross in range(8):
            for other in range(2):
                if cross or other:
                    last_hop(*unit, cross, other).wait()


def place(starts, goal, rows, out, totals, placer, got, made, in_sem, out_sem):
    steps = [(e, h, n) for e in range(2) for h in range(2) for n in range(4)]
    ins = [
        pltpu.make_async_copy(
            rows.at[h, e, :, n * PIECE : (n + 1) * PIECE], got.at[i], in_sem.at[i]
        )
        for i, (e, h, n) in enumerate(steps)
    ]
    outs = [
        pltpu.make_async_copy(
            made.at[i], out.at[e, :, pl.ds(h * HALF + n * PIECE, PIECE)], out_sem.at[i]
        )
        for i, (e, h, n) in enumerate(steps)
    ]
    for copy in ins:
        copy.start()
    line = lax.broadcasted_iota(jnp.int32, (WINDOW, 192), 0)
    for e in range(2):
        totals[e] = starts[8 + e, 0]
    for i, (e, h, n) in enumerate(steps):
        windows = [
            pl.multiple_of(jnp.minimum(starts[e * 4 + yy, 0] // 16 * 16, LINES - WINDOW), 16)
            for yy in range(4)
        ]
        if n == 0:
            for yy in range(4):
                mine = (h * 2 + e) * 4 + yy
                wanted = goal[mine : mine + 1, 0:192] - windows[yy]
                placer[yy] = jnp.where(wanted == line, 1.0, 0.0).astype(jnp.bfloat16)
        made[i, 192:] = jnp.zeros((LINES - 192, PIECE), jnp.bfloat16)
        ins[i].wait()
        for yy in range(4):
            part = jnp.dot(
                placer[yy], got[i, yy * 192 : (yy + 1) * 192, :], preferred_element_type=jnp.float32
            ).astype(jnp.bfloat16)
            if yy == 0:
                made[i, 0:WINDOW, :] = part
            else:
                shared = pl.ds(windows[yy], 16)
                made[i, shared, :] = made[i, shared, :] + part[:16]
                made[i, pl.ds(pl.multiple_of(windows[yy] + 16, 16), WINDOW - 16), :] = part[16:]
        outs[i].start()
    for copy in outs:
        copy.wait()


def shards(tokens, expert_ids):
    anywhere = pl.BlockSpec(memory_space=pl.ANY)
    vmem = pl.BlockSpec(memory_space=pltpu.VMEM)
    arrived, goal, starts = pl.pallas_call(
        exchange,
        out_shape=(
            jax.ShapeDtypeStruct((2, 2, LINES, HALF), jnp.bfloat16),
            jax.ShapeDtypeStruct((16, 256), jnp.int32),
            jax.ShapeDtypeStruct((16, TOK), jnp.int32),
        ),
        in_specs=[anywhere, vmem],
        out_specs=(anywhere, vmem, vmem),
        scratch_shapes=[
            pltpu.VMEM((2, 8, 2 * TOK, QUARTER), jnp.bfloat16),
            pltpu.VMEM((2, 2, 16, 96, 8 * TOK), jnp.bfloat16),
            pltpu.VMEM((2, 2, 2, 16, 2, 48, PIECE), jnp.bfloat16),
            pltpu.VMEM((2, 4, 3, 2, 2, 48, PIECE), jnp.bfloat16),
            pltpu.VMEM((2, 4, 2, 2, 2, 48, PIECE), jnp.bfloat16),
            pltpu.VMEM((256, TOK), jnp.float32),
            pltpu.VMEM((256, TOK), jnp.float32),
            pltpu.VMEM((2, 16, TOP, TOK), jnp.int32),
            pltpu.VMEM((8, 8, TOK), jnp.float32),
            pltpu.VMEM((8, 8, TOK), jnp.float32),
            pltpu.SemaphoreType.DMA((2,)),
            pltpu.SemaphoreType.DMA((2,)),
            pltpu.SemaphoreType.DMA((2,)),
            pltpu.SemaphoreType.DMA((2,)),
            pltpu.SemaphoreType.DMA((2, 16)),
            pltpu.SemaphoreType.DMA((2, 16)),
            pltpu.SemaphoreType.DMA((2, 2, 3, 2)),
            pltpu.SemaphoreType.DMA((2, 2, 3, 2)),
            pltpu.SemaphoreType.DMA((2, 2, 3, 8)),
            pltpu.SemaphoreType.DMA((2, 2, 3, 8)),
            pltpu.SemaphoreType.DMA((8,)),
            pltpu.SemaphoreType.DMA((8,)),
            pltpu.SemaphoreType.DMA((2, 4, 3)),
            pltpu.SemaphoreType.DMA((2, 4, 3)),
            pltpu.SemaphoreType.DMA((2, 4, 2)),
            pltpu.SemaphoreType.DMA((2, 4, 2)),
            pltpu.SemaphoreType.DMA((2, 4, 16)),
            pltpu.SemaphoreType.DMA((2, 4, 16)),
            pltpu.SemaphoreType.DMA((2, 4)),
        ],
        compiler_params=pltpu.CompilerParams(
            collective_id=0, has_side_effects=True, vmem_limit_bytes=67043328
        ),
        name="exchange",
    )(tokens, expert_ids.T)

    return pl.pallas_call(
        place,
        out_shape=(
            jax.ShapeDtypeStruct((2, LINES, WIDTH), jnp.bfloat16),
            jax.ShapeDtypeStruct((2,), jnp.int32),
        ),
        in_specs=[pl.BlockSpec(memory_space=pltpu.SMEM), vmem, anywhere],
        out_specs=(anywhere, pl.BlockSpec(memory_space=pltpu.SMEM)),
        scratch_shapes=[
            pltpu.VMEM((4, WINDOW, 192), jnp.bfloat16),
            pltpu.VMEM((16, LINES, PIECE), jnp.bfloat16),
            pltpu.VMEM((16, LINES, PIECE), jnp.bfloat16),
            pltpu.SemaphoreType.DMA((16,)),
            pltpu.SemaphoreType.DMA((16,)),
        ],
        compiler_params=pltpu.CompilerParams(vmem_limit_bytes=60 * 1024 * 1024),
        name="place",
    )(starts, goal, arrived)


def solution(mesh):
    in_specs = (P("ep", None), P("ep", None))
    out_specs = (P("ep", None, None), P("ep"))
    return jax.shard_map(shards, mesh=mesh, in_specs=in_specs, out_specs=out_specs, check_vma=False)
```

```python
import functools

import jax
import jax.numpy as jnp
from jax import lax
from jax.experimental import pallas as pl
from jax.experimental.pallas import tpu as pltpu
from jax.sharding import PartitionSpec as P

EXPERTS = 256
CAP = 6
TOP = 8
TOK = 128
WIDTH = 7168
HALF = WIDTH // 2
QUARTER = HALF // 2
PIECE = QUARTER // 2
LINES = 768
SPLITS = (((0, 384), (384, 256), (640, 256)), ((896, 256), (1152, 384), (1536, 256)))
MESH = pl.DeviceIdType.MESH
WINDOW = 208
ROUTES = ((1, 2, 4), (4, 2, 1), (1, 4, 2), (2, 1, 4))


def near(v):
    return v + 1 - 2 * (v % 2)


def far(v):
    return 3 - v


SHARE = (near, far)
CROSS = (far, near)
PAIR = (lambda v: v // 2, lambda v: ((v + 1) // 2) % 2)
MEMBER = (lambda v: v % 2, lambda v: v // 2)
SPOT = (lambda p, m: p * 2 + m, lambda p, m: p + m * (3 - 2 * p))


def pick(flag, flipped, value):
    return value + flag * (flipped - value)


def exchange(tok, ids, out, goal, starts, shared, via, onward, xg, oh, sb, mk, rk, idr, cts, ctr,
             load_sem, swap_send, swap_recv, id_sem, id_send, id_recv, own_send, own_recv,
             pass_send, pass_recv, count_send, count_recv, via_send, via_recv, onward_send,
             onward_recv, put_send, put_recv, keep_sem, fetch_sem):
    me = lax.axis_index("ep")
    core, x, z, y = me % 2, (me // 2) % 4, (me // 8) % 4, me // 32

    def device(yy, zz, xx, cc):
        return ((yy * 4 + zz) * 4 + xx) * 2 + cc

    def target(flip, d):
        return device(
            pick(d // 8, flip(y), y),
            pick((d // 4) % 2, flip(z), z),
            pick((d // 2) % 2, flip(x), x),
            pick(d % 2, 1 - core, core),
        )

    loads = []
    for h in range(2):
        loads.append(
            pltpu.make_async_copy(
                tok.at[:, pl.ds(pl.multiple_of(h * HALF + core * QUARTER, 128), QUARTER)],
                xg.at[h, 0, pl.ds(pl.multiple_of(core * TOK, TOK), TOK), :],
                load_sem.at[h],
            )
        )
        loads.append(pltpu.make_async_copy(ids, idr.at[h, 0], id_sem.at[h]))
    for copy in loads:
        copy.start()

    barrier = pltpu.get_barrier_semaphore()
    for h in range(2):
        for d in range(1, 16):
            if h == 0 or d >= 2:
                pl.semaphore_signal(
                    barrier, inc=1, device_id=(target(CROSS[h], d),), device_id_type=MESH
                )
    pl.semaphore_wait(barrier, 29)

    partner = device(y, z, x, 1 - core)
    swaps = []
    for h in range(2):
        copy = pltpu.make_async_remote_copy(
            src_ref=tok.at[:, pl.ds(pl.multiple_of(h * HALF + (1 - core) * QUARTER, 128), QUARTER)],
            dst_ref=xg.at[h, 0, pl.ds(pl.multiple_of(core * TOK, TOK), TOK), :],
            send_sem=swap_send.at[h],
            recv_sem=swap_recv.at[h],
            device_id=(partner,),
            device_id_type=MESH,
        )
        copy.start()
        swaps.append(copy)
    def neighbour(h, bit):
        flip = SHARE[h]
        if bit == 1:
            return device(y, z, flip(x), core)
        if bit == 2:
            return device(y, flip(z), x, core)
        return device(flip(y), z, x, core)

    def turns(i):
        return [(1, 2, 4)[(i + k) % 3] for k in range(3)]

    def give(h, n, i, step, other):
        at, size = SPLITS[n][i]
        cc = 1 - core if other else core
        bit = turns(i)[step]
        return pltpu.make_async_remote_copy(
            src_ref=tok.at[:, pl.ds(pl.multiple_of(h * HALF + cc * QUARTER + at, 128), size)],
            dst_ref=shared.at[h, bit, pl.ds(pl.multiple_of(core * TOK, TOK), TOK), pl.ds(at, size)],
            send_sem=own_send.at[h, n, i, step, other],
            recv_sem=own_recv.at[h, n, i, step, other],
            device_id=(neighbour(h, bit) + cc - core,),
            device_id_type=MESH,
        )

    def pass_on(h, n, i, kind):
        at, size = SPLITS[n][i]
        a, b, c = turns(i)
        slot, bit = ((a, b), (a, c), (b, c), (a | b, c))[kind]
        return pltpu.make_async_remote_copy(
            src_ref=shared.at[h, slot, :, pl.ds(at, size)],
            dst_ref=shared.at[h, slot | bit, :, pl.ds(at, size)],
            send_sem=pass_send.at[h, n, i, kind],
            recv_sem=pass_recv.at[h, n, i, kind],
            device_id=(neighbour(h, bit),),
            device_id_type=MESH,
        )

    both = [(h, i) for i in range(3) for h in range(2)]

    def give_all(n):
        for step in range(3):
            for h, i in both:
                for other in range(2):
                    give(h, n, i, step, other).start()

    def took(n, step):
        for h, i in both:
            for other in range(2):
                give(h, n, i, step, other).wait_recv()

    def pass_all(n, kind):
        for h, i in both:
            pass_on(h, n, i, kind).start()

    def passed(n, kind):
        for h, i in both:
            pass_on(h, n, i, kind).wait_recv()

    def fetch(h, n, g):
        cols = slice(n * PIECE, (n + 1) * PIECE)
        first = 1 if g == 0 else 4
        return pltpu.make_async_copy(
            shared.at[h, first : g * 4 + 4, :, cols],
            xg.at[h, first : g * 4 + 4, :, cols],
            fetch_sem.at[h, n, g],
        )

    sub = lax.broadcasted_iota(jnp.int32, (16, TOK), 0) % 8
    lane = lax.broadcasted_iota(jnp.int32, (8, TOK), 1)
    before = lax.broadcasted_iota(jnp.int32, (TOK, TOK), 0)
    after = lax.broadcasted_iota(jnp.int32, (TOK, TOK), 1)
    earlier = jnp.where(before < after, 1.0, 0.0).astype(jnp.bfloat16)
    ones = jnp.ones((TOK, TOK), jnp.bfloat16)

    def group_row(h, g):
        return pick(g, SHARE[h](y), y), PAIR[h](z) * 2 + PAIR[h](x)

    def source_place(h, k):
        return (
            pick(k // 4, 1 - MEMBER[h](z), MEMBER[h](z)) * 4
            + pick((k // 2) % 2, 1 - MEMBER[h](x), MEMBER[h](x)) * 2
            + k % 2
        )

    def build(h, g):
        slots = [(g * 4 + k // 2) * 2 + pick(k % 2, 1 - core, core) for k in range(8)]
        names = []
        for q in range(TOP):
            rows = jnp.zeros((8, TOK), jnp.int32)
            for k in range(8):
                rows = jnp.where(sub[:8] == source_place(h, k), idr[h, slots[k], q : q + 1, :], rows)
            names.append(rows)

        def marks(d, carry):
            owner = target(CROSS[h], d)
            for e in range(2):
                hit = names[0] == owner * 2 + e
                for q in range(1, TOP):
                    hit = hit | (names[q] == owner * 2 + e)
                mk[pl.ds(pl.multiple_of(d * 16 + e * 8, 8), 8), :] = jnp.where(hit, 1.0, 0.0)
            return carry

        lax.fori_loop(0, 16, marks, 0)
        marked = mk[...]
        whole = marked.astype(jnp.bfloat16)
        rank = jnp.dot(whole, earlier, preferred_element_type=jnp.float32)
        rk[...] = jnp.where(marked > 0.5, rank, -1.0)
        if h == 0:
            mk[...] = jnp.dot(whole, ones, preferred_element_type=jnp.float32)
            member = pick(g, 1 - y % 2, y % 2)
            for flips in range(8):
                tile = cts[flips]
                for e in range(2):
                    tile = jnp.where(
                        lane // 32 == member * 2 + e,
                        mk[flips * 32 + e * 8 : flips * 32 + e * 8 + 8, :],
                        tile,
                    )
                cts[flips] = tile

        def places(d, carry):
            for e in range(2):
                rank_e = rk[pl.ds(pl.multiple_of(d * 16 + e * 8, 8), 8), :]
                for j in range(0, CAP, 2):
                    hit = jnp.concatenate(
                        [jnp.where(rank_e == float(j + q), 1.0, 0.0) for q in range(2)], axis=0
                    )
                    for k in range(8):
                        oh[h, g, d, e * 48 + j * 8 : e * 48 + j * 8 + 16, k * TOK : (k + 1) * TOK] = (
                            jnp.where(sub == source_place(h, k), hit, 0.0).astype(jnp.bfloat16)
                        )
            return carry

        lax.fori_loop(0, 16, places, 0)

    give_all(0)
    names_sent = []
    for d in range(1, 16):
        for h in range(2):
            copy = pltpu.make_async_remote_copy(
                src_ref=ids,
                dst_ref=idr.at[h, d],
                send_sem=id_send.at[h, d],
                recv_sem=id_recv.at[h, d],
                device_id=(target(SHARE[h], d),),
                device_id_type=MESH,
            )
            copy.start()
            names_sent.append(copy)

    cts[...] = jnp.zeros(cts.shape, jnp.float32)
    took(0, 0)
    pass_all(0, 0)
    pass_all(0, 1)
    took(0, 1)
    pass_all(0, 2)
    for copy in loads:
        copy.wait()
    for copy in swaps:
        copy.wait_recv()
    for copy in names_sent:
        copy.wait_recv()
    build(0, 0)
    passed(0, 0)
    pass_all(0, 3)
    give_all(1)
    took(1, 0)
    pass_all(1, 0)
    pass_all(1, 1)
    took(1, 1)
    pass_all(1, 2)
    build(0, 1)
    passed(1, 0)
    pass_all(1, 3)

    block = (y // 2) * 4 + (z // 2) * 2 + x // 2
    counts = []
    for flips in range(1, 8):
        copy = pltpu.make_async_remote_copy(
            src_ref=cts.at[flips],
            dst_ref=ctr.at[block],
            send_sem=count_send.at[flips],
            recv_sem=count_recv.at[flips],
            device_id=(target(far, flips * 2),),
            device_id_type=MESH,
        )
        copy.start()
        counts.append(copy)
    own_count = pltpu.make_async_copy(cts.at[0], ctr.at[block], count_send.at[0])
    own_count.start()
    build(1, 0)
    build(1, 1)

    def shift(h, bits):
        flip = CROSS[h]
        return (
            flip(y) if bits & 4 else y,
            flip(z) if bits & 2 else z,
            flip(x) if bits & 1 else x,
        )

    def landing(h, n, g, done):
        yy, zz, xx = shift(h, done)
        ys = SHARE[h](yy) if g else yy
        where = PAIR[h](zz) * 2 + PAIR[h](xx)
        return out.at[
            h,
            :,
            pl.ds(pl.multiple_of(ys * 192 + where * 48, 16), 48),
            pl.ds(pl.multiple_of(core * QUARTER + n * PIECE, 128), PIECE),
        ]

    def route(n, g):
        return ROUTES[n * 2 + g]

    def last_hop(h, n, g, cross, other):
        a, b, c = route(n, g)
        chunk = n * 2 + g
        bit = {a: a, b: b, a | b: b}.get(cross, 0 if cross == 0 else c)
        done = cross ^ bit
        if done == 0:
            src = sb.at[h, n, g, cross * 2 + other]
        elif done == a:
            src = via.at[h, chunk, 0 if cross == a | b else 1, other]
        else:
            src = onward.at[h, chunk, 0 if done == b else 1, other]
        return pltpu.make_async_remote_copy(
            src_ref=src,
            dst_ref=landing(h, n, g, done),
            send_sem=put_send.at[h, chunk, cross * 2 + other],
            recv_sem=put_recv.at[h, chunk, cross * 2 + other],
            device_id=(device(*shift(h, bit), 1 - core if other else core),),
            device_id_type=MESH,
        )

    def first_hop(h, n, g, which):
        a, b, c = route(n, g)
        cross = (a | b, a | c, a | b | c)[which]
        return pltpu.make_async_remote_copy(
            src_ref=sb.at[h, n, g, pl.ds(cross * 2, 2)],
            dst_ref=via.at[h, n * 2 + g, which],
            send_sem=via_send.at[h, n * 2 + g, which],
            recv_sem=via_recv.at[h, n * 2 + g, which],
            device_id=(device(*shift(h, a), core),),
            device_id_type=MESH,
        )

    def next_hop(h, n, g, which):
        a, b, c = route(n, g)
        chunk = n * 2 + g
        return pltpu.make_async_remote_copy(
            src_ref=sb.at[h, n, g, pl.ds((b | c) * 2, 2)] if which == 0 else via.at[h, chunk, 2],
            dst_ref=onward.at[h, chunk, which],
            send_sem=onward_send.at[h, chunk, which],
            recv_sem=onward_recv.at[h, chunk, which],
            device_id=(device(*shift(h, b), core),),
            device_id_type=MESH,
        )

    def keep(h, n, g):
        return pltpu.make_async_copy(
            sb.at[h, n, g, 0], landing(h, n, g, 0), keep_sem.at[h, n * 2 + g]
        )

    def pack(h, n, g):
        def some(m, carry):
            placer = oh[h, g, pl.ds(m * 4, 4)].reshape(384, 1024)
            rows = xg[h, g * 4 : g * 4 + 4, :, n * PIECE : (n + 1) * PIECE]
            packed = jnp.dot(placer, rows.reshape(1024, PIECE), preferred_element_type=jnp.float32)
            sb[h, n, g, pl.ds(m * 4, 4)] = packed.astype(jnp.bfloat16).reshape(4, 2, 48, PIECE)
            return carry

        lax.fori_loop(0, 4, some, 0)

    def leave(h, n, g):
        for which in (2, 0, 1):
            first_hop(h, n, g, which).start()
        next_hop(h, n, g, 0).start()
        keep(h, n, g).start()
        last_hop(h, n, g, 0, 1).start()

    def direct(h, n, g):
        for cross in route(n, g):
            for other in range(2):
                last_hop(h, n, g, cross, other).start()

    def relay(h, n, g):
        a, b, c = route(n, g)
        first_hop(h, n, g, 2).wait_recv()
        next_hop(h, n, g, 1).start()
        for which, cross in ((0, a | b), (1, a | c)):
            first_hop(h, n, g, which).wait_recv()
            for other in range(2):
                last_hop(h, n, g, cross, other).start()
        if n == 1:
            direct(h, n, g)

    def finish(h, n, g):
        a, b, c = route(n, g)
        for which, cross in ((0, b | c), (1, a | b | c)):
            next_hop(h, n, g, which).wait_recv()
            for other in range(2):
                last_hop(h, n, g, cross, other).start()

    units = [(h, n, g) for n in range(2) for g in range(2) for h in range(2)]

    def gather(n):
        took(n, 2)
        for kind in range(1, 4):
            passed(n, kind)
        for g in range(2):
            for h in range(2):
                fetch(h, n, g).start()

    gather(0)
    for i in range(4):
        h, n, g = units[i]
        fetch(h, n, g).wait()
        pack(h, n, g)
        if i > 0:
            leave(*units[i - 1])
            direct(*units[i - 1])

    own_count.wait()
    for copy in counts:
        copy.wait_recv()
    table = ctr[...].reshape(64, TOK).astype(jnp.bfloat16)
    row = lax.broadcasted_iota(jnp.int32, (64, 192), 0)
    col = lax.broadcasted_iota(jnp.int32, (64, 192), 1)
    row_z = SPOT[0]((row // 16) % 2, (row // 4) % 2)
    row_x = SPOT[0]((row // 8) % 2, (row // 2) % 2)
    turn = (((0,), (0,)), ((), ()))
    slot = (lax.broadcasted_iota(jnp.int32, (1, 192), 1) % 48) // 8
    for h in range(2):
        col_z = SPOT[h](col // 96, (col % 8) // 4)
        col_x = SPOT[h]((col // 48) % 2, (col // 2) % 2)
        for yy in range(4):
            there = device(yy, col_z, col_x, col % 2)
            base = [jnp.zeros((1, 192), jnp.float32) for _ in range(2)]
            have = [jnp.zeros((1, 192), jnp.float32) for _ in range(2)]
            for member in range(2):
                here = device((row // 32) * 2 + member, row_z, row_x, row % 2)
                below = jnp.where(here < there, 1.0, 0.0).astype(jnp.bfloat16)
                same = jnp.where(here == there, 1.0, 0.0).astype(jnp.bfloat16)
                below = lax.dot_general(table, below, turn, preferred_element_type=jnp.float32)
                same = lax.dot_general(table, same, turn, preferred_element_type=jnp.float32)
                for e in range(2):
                    at = member * 64 + e * 32
                    base[e] = base[e] + below[at : at + 1, :]
                    have[e] = have[e] + same[at : at + 1, :]
            for e in range(2):
                at = base[e].astype(jnp.int32)
                mine = (h * 2 + e) * 4 + yy
                goal[mine : mine + 1, 0:192] = jnp.where(slot < have[e].astype(jnp.int32), at + slot, -1)
                if h == 0:
                    starts[e * 4 + yy : e * 4 + yy + 1, :] = at[:, 0:TOK]
    sums = lax.dot_general(
        table, jnp.ones((64, TOK), jnp.bfloat16), turn, preferred_element_type=jnp.float32
    )
    for e in range(2):
        starts[8 + e : 9 + e, :] = (
            sums[e * 32 : e * 32 + 1, :] + sums[64 + e * 32 : 65 + e * 32, :]
        ).astype(jnp.int32)

    leave(*units[3])
    direct(*units[3])
    gather(1)
    for i in range(4, 8):
        h, n, g = units[i]
        fetch(h, n, g).wait()
        pack(h, n, g)
        if i > 4:
            leave(*units[i - 1])
        relay(*units[i - 4])
    finish(*units[0])
    leave(*units[7])
    finish(*units[1])
    for at in (4, 6):
        relay(*units[at])
        relay(*units[at + 1])
        finish(*units[at - 2])
        finish(*units[at - 1])
    finish(*units[6])
    finish(*units[7])

    for copy in names_sent + counts + swaps:
        copy.wait_send()
    for n in range(2):
        for h, i in both:
            for step in range(3):
                for other in range(2):
                    give(h, n, i, step, other).wait_send()
            for kind in range(4):
                pass_on(h, n, i, kind).wait_send()
    for unit in units:
        for which in range(3):
            first_hop(*unit, which).wait_send()
        for which in range(2):
            next_hop(*unit, which).wait_send()
        keep(*unit).wait()
        for cross in range(8):
            for other in range(2):
                if cross or other:
                    last_hop(*unit, cross, other).wait()


def place(starts, goal, rows, out, totals, placer, got, made, in_sem, out_sem):
    steps = [(e, h, n) for e in range(2) for h in range(2) for n in range(4)]
    ins = [
        pltpu.make_async_copy(
            rows.at[h, e, :, n * PIECE : (n + 1) * PIECE], got.at[i], in_sem.at[i]
        )
        for i, (e, h, n) in enumerate(steps)
    ]
    outs = [
        pltpu.make_async_copy(
            made.at[i], out.at[e, :, pl.ds(h * HALF + n * PIECE, PIECE)], out_sem.at[i]
        )
        for i, (e, h, n) in enumerate(steps)
    ]
    for copy in ins:
        copy.start()
    line = lax.broadcasted_iota(jnp.int32, (WINDOW, 192), 0)
    for e in range(2):
        totals[e] = starts[8 + e, 0]
    for i, (e, h, n) in enumerate(steps):
        windows = [
            pl.multiple_of(jnp.minimum(starts[e * 4 + yy, 0] // 16 * 16, LINES - WINDOW), 16)
            for yy in range(4)
        ]
        if n == 0:
            for yy in range(4):
                mine = (h * 2 + e) * 4 + yy
                wanted = goal[mine : mine + 1, 0:192] - windows[yy]
                placer[yy] = jnp.where(wanted == line, 1.0, 0.0).astype(jnp.bfloat16)
        made[i, 192:] = jnp.zeros((LINES - 192, PIECE), jnp.bfloat16)
        ins[i].wait()
        for yy in range(4):
            part = jnp.dot(
                placer[yy], got[i, yy * 192 : (yy + 1) * 192, :], preferred_element_type=jnp.float32
            ).astype(jnp.bfloat16)
            if yy == 0:
                made[i, 0:WINDOW, :] = part
            else:
                shared = pl.ds(windows[yy], 16)
                made[i, shared, :] = made[i, shared, :] + part[:16]
                made[i, pl.ds(pl.multiple_of(windows[yy] + 16, 16), WINDOW - 16), :] = part[16:]
        outs[i].start()
    for copy in outs:
        copy.wait()


def shards(tokens, expert_ids):
    anywhere = pl.BlockSpec(memory_space=pl.ANY)
    vmem = pl.BlockSpec(memory_space=pltpu.VMEM)
    arrived, goal, starts, *_ = pl.pallas_call(
        exchange,
        out_shape=(
            jax.ShapeDtypeStruct((2, 2, LINES, HALF), jnp.bfloat16),
            jax.ShapeDtypeStruct((16, 256), jnp.int32),
            jax.ShapeDtypeStruct((16, TOK), jnp.int32),
            jax.ShapeDtypeStruct((2, 8, 2 * TOK, QUARTER), jnp.bfloat16),
            jax.ShapeDtypeStruct((2, 4, 3, 2, 2, 48, PIECE), jnp.bfloat16),
            jax.ShapeDtypeStruct((2, 4, 2, 2, 2, 48, PIECE), jnp.bfloat16),
        ),
        in_specs=[anywhere, vmem],
        out_specs=(anywhere, vmem, vmem, anywhere, anywhere, anywhere),
        scratch_shapes=[
            pltpu.VMEM((2, 8, 2 * TOK, QUARTER), jnp.bfloat16),
            pltpu.VMEM((2, 2, 16, 96, 8 * TOK), jnp.bfloat16),
            pltpu.VMEM((2, 2, 2, 16, 2, 48, PIECE), jnp.bfloat16),
            pltpu.VMEM((256, TOK), jnp.float32),
            pltpu.VMEM((256, TOK), jnp.float32),
            pltpu.VMEM((2, 16, TOP, TOK), jnp.int32),
            pltpu.VMEM((8, 8, TOK), jnp.float32),
            pltpu.VMEM((8, 8, TOK), jnp.float32),
            pltpu.SemaphoreType.DMA((2,)),
            pltpu.SemaphoreType.DMA((2,)),
            pltpu.SemaphoreType.DMA((2,)),
            pltpu.SemaphoreType.DMA((2,)),
            pltpu.SemaphoreType.DMA((2, 16)),
            pltpu.SemaphoreType.DMA((2, 16)),
            pltpu.SemaphoreType.DMA((2, 2, 3, 3, 2)),
            pltpu.SemaphoreType.DMA((2, 2, 3, 3, 2)),
            pltpu.SemaphoreType.DMA((2, 2, 3, 4)),
            pltpu.SemaphoreType.DMA((2, 2, 3, 4)),
            pltpu.SemaphoreType.DMA((8,)),
            pltpu.SemaphoreType.DMA((8,)),
            pltpu.SemaphoreType.DMA((2, 4, 3)),
            pltpu.SemaphoreType.DMA((2, 4, 3)),
            pltpu.SemaphoreType.DMA((2, 4, 2)),
            pltpu.SemaphoreType.DMA((2, 4, 2)),
            pltpu.SemaphoreType.DMA((2, 4, 16)),
            pltpu.SemaphoreType.DMA((2, 4, 16)),
            pltpu.SemaphoreType.DMA((2, 4)),
            pltpu.SemaphoreType.DMA((2, 2, 2)),
        ],
        compiler_params=pltpu.CompilerParams(
            collective_id=0, has_side_effects=True, vmem_limit_bytes=60 * 1024 * 1024
        ),
        name="exchange",
    )(tokens, expert_ids.T)

    return pl.pallas_call(
        place,
        out_shape=(
            jax.ShapeDtypeStruct((2, LINES, WIDTH), jnp.bfloat16),
            jax.ShapeDtypeStruct((2,), jnp.int32),
        ),
        in_specs=[pl.BlockSpec(memory_space=pltpu.SMEM), vmem, anywhere],
        out_specs=(anywhere, pl.BlockSpec(memory_space=pltpu.SMEM)),
        scratch_shapes=[
            pltpu.VMEM((4, WINDOW, 192), jnp.bfloat16),
            pltpu.VMEM((16, LINES, PIECE), jnp.bfloat16),
            pltpu.VMEM((16, LINES, PIECE), jnp.bfloat16),
            pltpu.SemaphoreType.DMA((16,)),
            pltpu.SemaphoreType.DMA((16,)),
        ],
        compiler_params=pltpu.CompilerParams(vmem_limit_bytes=60 * 1024 * 1024),
        name="place",
    )(starts, goal, arrived)


def solution(mesh):
    in_specs = (P("ep", None), P("ep", None))
    out_specs = (P("ep", None, None), P("ep"))
    return jax.shard_map(shards, mesh=mesh, in_specs=in_specs, out_specs=out_specs, check_vma=False)
```

```python
import functools

import jax
import jax.numpy as jnp
from jax import lax
from jax.experimental import pallas as pl
from jax.experimental.pallas import tpu as pltpu
from jax.sharding import PartitionSpec as P

EXPERTS = 256
CAP = 6
TOP = 8
TOK = 128
WIDTH = 7168
HALF = WIDTH // 2
QUARTER = HALF // 2
PIECE = QUARTER // 2
LINES = 768
SPLITS = (((0, 384), (384, 256), (640, 256)), ((896, 256), (1152, 384), (1536, 256)))
MESH = pl.DeviceIdType.MESH
WINDOW = 208
ROUTES = ((1, 2, 4), (4, 2, 1), (1, 4, 2), (2, 1, 4))


def near(v):
    return v + 1 - 2 * (v % 2)


def far(v):
    return 3 - v


SHARE = (near, far)
CROSS = (far, near)
PAIR = (lambda v: v // 2, lambda v: ((v + 1) // 2) % 2)
MEMBER = (lambda v: v % 2, lambda v: v // 2)
SPOT = (lambda p, m: p * 2 + m, lambda p, m: p + m * (3 - 2 * p))


def pick(flag, flipped, value):
    return value + flag * (flipped - value)


def exchange(tok, ids, out, goal, starts, shared, via, onward, xg, oh, sb, mk, rk, idr, cts, ctr,
             load_sem, swap_send, swap_recv, id_sem, id_send, id_recv, own_send, own_recv,
             pass_send, pass_recv, count_send, count_recv, via_send, via_recv, onward_send,
             onward_recv, put_send, put_recv, keep_sem, fetch_sem):
    me = lax.axis_index("ep")
    core, x, z, y = me % 2, (me // 2) % 4, (me // 8) % 4, me // 32

    def device(yy, zz, xx, cc):
        return ((yy * 4 + zz) * 4 + xx) * 2 + cc

    def target(flip, d):
        return device(
            pick(d // 8, flip(y), y),
            pick((d // 4) % 2, flip(z), z),
            pick((d // 2) % 2, flip(x), x),
            pick(d % 2, 1 - core, core),
        )

    loads = []
    for h in range(2):
        loads.append(
            pltpu.make_async_copy(
                tok.at[:, pl.ds(pl.multiple_of(h * HALF + core * QUARTER, 128), QUARTER)],
                xg.at[h, 0, pl.ds(pl.multiple_of(core * TOK, TOK), TOK), :],
                load_sem.at[h],
            )
        )
        loads.append(pltpu.make_async_copy(ids, idr.at[h, 0], id_sem.at[h]))
    for copy in loads:
        copy.start()

    barrier = pltpu.get_barrier_semaphore()
    for h in range(2):
        for d in range(1, 16):
            if h == 0 or d >= 2:
                pl.semaphore_signal(
                    barrier, inc=1, device_id=(target(CROSS[h], d),), device_id_type=MESH
                )
    pl.semaphore_wait(barrier, 29)

    partner = device(y, z, x, 1 - core)
    swaps = []
    for h in range(2):
        copy = pltpu.make_async_remote_copy(
            src_ref=tok.at[:, pl.ds(pl.multiple_of(h * HALF + (1 - core) * QUARTER, 128), QUARTER)],
            dst_ref=xg.at[h, 0, pl.ds(pl.multiple_of(core * TOK, TOK), TOK), :],
            send_sem=swap_send.at[h],
            recv_sem=swap_recv.at[h],
            device_id=(partner,),
            device_id_type=MESH,
        )
        copy.start()
        swaps.append(copy)
    def neighbour(h, bit):
        flip = SHARE[h]
        if bit == 1:
            return device(y, z, flip(x), core)
        if bit == 2:
            return device(y, flip(z), x, core)
        return device(flip(y), z, x, core)

    def turns(i):
        return [(1, 2, 4)[(i + k) % 3] for k in range(3)]

    def give(h, n, i, step, other):
        at, size = SPLITS[n][i]
        cc = 1 - core if other else core
        bit = turns(i)[step]
        return pltpu.make_async_remote_copy(
            src_ref=tok.at[:, pl.ds(pl.multiple_of(h * HALF + cc * QUARTER + at, 128), size)],
            dst_ref=shared.at[h, bit, pl.ds(pl.multiple_of(core * TOK, TOK), TOK), pl.ds(at, size)],
            send_sem=own_send.at[h, n, i, step, other],
            recv_sem=own_recv.at[h, n, i, step, other],
            device_id=(neighbour(h, bit) + cc - core,),
            device_id_type=MESH,
        )

    def pass_on(h, n, i, kind):
        at, size = SPLITS[n][i]
        a, b, c = turns(i)
        slot, bit = ((a, b), (a, c), (b, c), (a | b, c))[kind]
        return pltpu.make_async_remote_copy(
            src_ref=shared.at[h, slot, :, pl.ds(at, size)],
            dst_ref=shared.at[h, slot | bit, :, pl.ds(at, size)],
            send_sem=pass_send.at[h, n, i, kind],
            recv_sem=pass_recv.at[h, n, i, kind],
            device_id=(neighbour(h, bit),),
            device_id_type=MESH,
        )

    both = [(h, i) for i in range(3) for h in range(2)]

    def give_all(n):
        for step in range(3):
            for h, i in both:
                for other in range(2):
                    give(h, n, i, step, other).start()

    def took(n, step):
        for h, i in both:
            for other in range(2):
                give(h, n, i, step, other).wait_recv()

    def pass_all(n, kind):
        for h, i in both:
            pass_on(h, n, i, kind).start()

    def passed(n, kind):
        for h, i in both:
            pass_on(h, n, i, kind).wait_recv()

    def fetch(h, n, g):
        cols = slice(n * PIECE, (n + 1) * PIECE)
        first = 1 if g == 0 else 4
        return pltpu.make_async_copy(
            shared.at[h, first : g * 4 + 4, :, cols],
            xg.at[h, first : g * 4 + 4, :, cols],
            fetch_sem.at[h, n, g],
        )

    sub = lax.broadcasted_iota(jnp.int32, (16, TOK), 0) % 8
    lane = lax.broadcasted_iota(jnp.int32, (8, TOK), 1)
    before = lax.broadcasted_iota(jnp.int32, (TOK, TOK), 0)
    after = lax.broadcasted_iota(jnp.int32, (TOK, TOK), 1)
    earlier = jnp.where(before < after, 1.0, 0.0).astype(jnp.bfloat16)
    ones = jnp.ones((TOK, TOK), jnp.bfloat16)

    def group_row(h, g):
        return pick(g, SHARE[h](y), y), PAIR[h](z) * 2 + PAIR[h](x)

    def source_place(h, k):
        return (
            pick(k // 4, 1 - MEMBER[h](z), MEMBER[h](z)) * 4
            + pick((k // 2) % 2, 1 - MEMBER[h](x), MEMBER[h](x)) * 2
            + k % 2
        )

    def build(h, g):
        slots = [(g * 4 + k // 2) * 2 + pick(k % 2, 1 - core, core) for k in range(8)]
        names = []
        for q in range(TOP):
            rows = jnp.zeros((8, TOK), jnp.int32)
            for k in range(8):
                rows = jnp.where(sub[:8] == source_place(h, k), idr[h, slots[k], q : q + 1, :], rows)
            names.append(rows)

        def marks(d, carry):
            owner = target(CROSS[h], d)
            for e in range(2):
                hit = names[0] == owner * 2 + e
                for q in range(1, TOP):
                    hit = hit | (names[q] == owner * 2 + e)
                mk[pl.ds(pl.multiple_of(d * 16 + e * 8, 8), 8), :] = jnp.where(hit, 1.0, 0.0)
            return carry

        lax.fori_loop(0, 16, marks, 0)
        marked = mk[...]
        whole = marked.astype(jnp.bfloat16)
        rank = jnp.dot(whole, earlier, preferred_element_type=jnp.float32)
        rk[...] = jnp.where(marked > 0.5, rank, -1.0)
        if h == 0:
            mk[...] = jnp.dot(whole, ones, preferred_element_type=jnp.float32)
            member = pick(g, 1 - y % 2, y % 2)
            for flips in range(8):
                tile = cts[flips]
                for e in range(2):
                    tile = jnp.where(
                        lane // 32 == member * 2 + e,
                        mk[flips * 32 + e * 8 : flips * 32 + e * 8 + 8, :],
                        tile,
                    )
                cts[flips] = tile

        def places(d, carry):
            for e in range(2):
                rank_e = rk[pl.ds(pl.multiple_of(d * 16 + e * 8, 8), 8), :]
                for j in range(0, CAP, 2):
                    hit = jnp.concatenate(
                        [jnp.where(rank_e == float(j + q), 1.0, 0.0) for q in range(2)], axis=0
                    )
                    for k in range(8):
                        oh[h, g, d, e * 48 + j * 8 : e * 48 + j * 8 + 16, k * TOK : (k + 1) * TOK] = (
                            jnp.where(sub == source_place(h, k), hit, 0.0).astype(jnp.bfloat16)
                        )
            return carry

        lax.fori_loop(0, 16, places, 0)

    give_all(0)
    names_sent = []
    for d in range(1, 16):
        for h in range(2):
            copy = pltpu.make_async_remote_copy(
                src_ref=ids,
                dst_ref=idr.at[h, d],
                send_sem=id_send.at[h, d],
                recv_sem=id_recv.at[h, d],
                device_id=(target(SHARE[h], d),),
                device_id_type=MESH,
            )
            copy.start()
            names_sent.append(copy)

    cts[...] = jnp.zeros(cts.shape, jnp.float32)
    took(0, 0)
    pass_all(0, 0)
    pass_all(0, 1)
    took(0, 1)
    pass_all(0, 2)
    for copy in loads:
        copy.wait()
    for copy in swaps:
        copy.wait_recv()
    passed(0, 0)
    pass_all(0, 3)
    give_all(1)
    for copy in names_sent:
        copy.wait_recv()
    build(0, 0)
    took(1, 0)
    pass_all(1, 0)
    pass_all(1, 1)
    took(1, 1)
    pass_all(1, 2)
    build(0, 1)
    passed(1, 0)
    pass_all(1, 3)

    block = (y // 2) * 4 + (z // 2) * 2 + x // 2
    counts = []
    for flips in range(1, 8):
        copy = pltpu.make_async_remote_copy(
            src_ref=cts.at[flips],
            dst_ref=ctr.at[block],
            send_sem=count_send.at[flips],
            recv_sem=count_recv.at[flips],
            device_id=(target(far, flips * 2),),
            device_id_type=MESH,
        )
        copy.start()
        counts.append(copy)
    own_count = pltpu.make_async_copy(cts.at[0], ctr.at[block], count_send.at[0])
    own_count.start()
    build(1, 0)
    build(1, 1)

    def shift(h, bits):
        flip = CROSS[h]
        return (
            flip(y) if bits & 4 else y,
            flip(z) if bits & 2 else z,
            flip(x) if bits & 1 else x,
        )

    def landing(h, n, g, done):
        yy, zz, xx = shift(h, done)
        ys = SHARE[h](yy) if g else yy
        where = PAIR[h](zz) * 2 + PAIR[h](xx)
        return out.at[
            h,
            :,
            pl.ds(pl.multiple_of(ys * 192 + where * 48, 16), 48),
            pl.ds(pl.multiple_of(core * QUARTER + n * PIECE, 128), PIECE),
        ]

    def route(n, g):
        return ROUTES[n * 2 + g]

    def last_hop(h, n, g, cross, other):
        a, b, c = route(n, g)
        chunk = n * 2 + g
        bit = {a: a, b: b, a | b: b}.get(cross, 0 if cross == 0 else c)
        done = cross ^ bit
        if done == 0:
            src = sb.at[h, n, g, cross * 2 + other]
        elif done == a:
            src = via.at[h, chunk, 0 if cross == a | b else 1, other]
        else:
            src = onward.at[h, chunk, 0 if done == b else 1, other]
        return pltpu.make_async_remote_copy(
            src_ref=src,
            dst_ref=landing(h, n, g, done),
            send_sem=put_send.at[h, chunk, cross * 2 + other],
            recv_sem=put_recv.at[h, chunk, cross * 2 + other],
            device_id=(device(*shift(h, bit), 1 - core if other else core),),
            device_id_type=MESH,
        )

    def first_hop(h, n, g, which):
        a, b, c = route(n, g)
        cross = (a | b, a | c, a | b | c)[which]
        return pltpu.make_async_remote_copy(
            src_ref=sb.at[h, n, g, pl.ds(cross * 2, 2)],
            dst_ref=via.at[h, n * 2 + g, which],
            send_sem=via_send.at[h, n * 2 + g, which],
            recv_sem=via_recv.at[h, n * 2 + g, which],
            device_id=(device(*shift(h, a), core),),
            device_id_type=MESH,
        )

    def next_hop(h, n, g, which):
        a, b, c = route(n, g)
        chunk = n * 2 + g
        return pltpu.make_async_remote_copy(
            src_ref=sb.at[h, n, g, pl.ds((b | c) * 2, 2)] if which == 0 else via.at[h, chunk, 2],
            dst_ref=onward.at[h, chunk, which],
            send_sem=onward_send.at[h, chunk, which],
            recv_sem=onward_recv.at[h, chunk, which],
            device_id=(device(*shift(h, b), core),),
            device_id_type=MESH,
        )

    def keep(h, n, g):
        return pltpu.make_async_copy(
            sb.at[h, n, g, 0], landing(h, n, g, 0), keep_sem.at[h, n * 2 + g]
        )

    def pack(h, n, g):
        def some(m, carry):
            placer = oh[h, g, pl.ds(m * 4, 4)].reshape(384, 1024)
            rows = xg[h, g * 4 : g * 4 + 4, :, n * PIECE : (n + 1) * PIECE]
            packed = jnp.dot(placer, rows.reshape(1024, PIECE), preferred_element_type=jnp.float32)
            sb[h, n, g, pl.ds(m * 4, 4)] = packed.astype(jnp.bfloat16).reshape(4, 2, 48, PIECE)
            return carry

        lax.fori_loop(0, 4, some, 0)

    def leave(h, n, g):
        for which in (2, 0, 1):
            first_hop(h, n, g, which).start()
        next_hop(h, n, g, 0).start()
        keep(h, n, g).start()
        last_hop(h, n, g, 0, 1).start()

    def direct(h, n, g):
        for cross in route(n, g):
            for other in range(2):
                last_hop(h, n, g, cross, other).start()

    def relay(h, n, g):
        a, b, c = route(n, g)
        first_hop(h, n, g, 2).wait_recv()
        next_hop(h, n, g, 1).start()
        for which, cross in ((0, a | b), (1, a | c)):
            first_hop(h, n, g, which).wait_recv()
            for other in range(2):
                last_hop(h, n, g, cross, other).start()
        if n == 1:
            direct(h, n, g)

    def finish(h, n, g):
        a, b, c = route(n, g)
        for which, cross in ((0, b | c), (1, a | b | c)):
            next_hop(h, n, g, which).wait_recv()
            for other in range(2):
                last_hop(h, n, g, cross, other).start()

    units = [(h, n, g) for n in range(2) for g in range(2) for h in range(2)]

    def gather(n):
        took(n, 2)
        for kind in range(1, 4):
            passed(n, kind)
        for g in range(2):
            for h in range(2):
                fetch(h, n, g).start()

    gather(0)
    for i in range(4):
        h, n, g = units[i]
        fetch(h, n, g).wait()
        pack(h, n, g)
        if i > 0:
            leave(*units[i - 1])
            direct(*units[i - 1])

    leave(*units[3])
    direct(*units[3])
    gather(1)
    for i in range(4, 8):
        h, n, g = units[i]
        fetch(h, n, g).wait()
        pack(h, n, g)
        if i > 4:
            leave(*units[i - 1])
        relay(*units[i - 4])
    finish(*units[0])
    leave(*units[7])
    finish(*units[1])
    own_count.wait()
    for copy in counts:
        copy.wait_recv()
    table = ctr[...].reshape(64, TOK).astype(jnp.bfloat16)
    row = lax.broadcasted_iota(jnp.int32, (64, 192), 0)
    col = lax.broadcasted_iota(jnp.int32, (64, 192), 1)
    row_z = SPOT[0]((row // 16) % 2, (row // 4) % 2)
    row_x = SPOT[0]((row // 8) % 2, (row // 2) % 2)
    turn = (((0,), (0,)), ((), ()))
    slot = (lax.broadcasted_iota(jnp.int32, (1, 192), 1) % 48) // 8
    for h in range(2):
        col_z = SPOT[h](col // 96, (col % 8) // 4)
        col_x = SPOT[h]((col // 48) % 2, (col // 2) % 2)
        for yy in range(4):
            there = device(yy, col_z, col_x, col % 2)
            base = [jnp.zeros((1, 192), jnp.float32) for _ in range(2)]
            have = [jnp.zeros((1, 192), jnp.float32) for _ in range(2)]
            for member in range(2):
                here = device((row // 32) * 2 + member, row_z, row_x, row % 2)
                below = jnp.where(here < there, 1.0, 0.0).astype(jnp.bfloat16)
                same = jnp.where(here == there, 1.0, 0.0).astype(jnp.bfloat16)
                below = lax.dot_general(table, below, turn, preferred_element_type=jnp.float32)
                same = lax.dot_general(table, same, turn, preferred_element_type=jnp.float32)
                for e in range(2):
                    at = member * 64 + e * 32
                    base[e] = base[e] + below[at : at + 1, :]
                    have[e] = have[e] + same[at : at + 1, :]
            for e in range(2):
                at = base[e].astype(jnp.int32)
                mine = (h * 2 + e) * 4 + yy
                goal[mine : mine + 1, 0:192] = jnp.where(slot < have[e].astype(jnp.int32), at + slot, -1)
                if h == 0:
                    starts[e * 4 + yy : e * 4 + yy + 1, :] = at[:, 0:TOK]
    sums = lax.dot_general(
        table, jnp.ones((64, TOK), jnp.bfloat16), turn, preferred_element_type=jnp.float32
    )
    for e in range(2):
        starts[8 + e : 9 + e, :] = (
            sums[e * 32 : e * 32 + 1, :] + sums[64 + e * 32 : 65 + e * 32, :]
        ).astype(jnp.int32)

    for at in (4, 6):
        relay(*units[at])
        relay(*units[at + 1])
        finish(*units[at - 2])
        finish(*units[at - 1])
    finish(*units[6])
    finish(*units[7])

    for copy in names_sent + counts + swaps:
        copy.wait_send()
    for n in range(2):
        for h, i in both:
            for step in range(3):
                for other in range(2):
                    give(h, n, i, step, other).wait_send()
            for kind in range(4):
                pass_on(h, n, i, kind).wait_send()
    for unit in units:
        for which in range(3):
            first_hop(*unit, which).wait_send()
        for which in range(2):
            next_hop(*unit, which).wait_send()
        keep(*unit).wait()
        for cross in range(8):
            for other in range(2):
                if cross or other:
                    last_hop(*unit, cross, other).wait()


def place(starts, goal, rows, out, totals, placer, got, made, in_sem, out_sem):
    steps = [(e, h, n) for e in range(2) for h in range(2) for n in range(4)]
    ins = [
        pltpu.make_async_copy(
            rows.at[h, e, :, n * PIECE : (n + 1) * PIECE], got.at[i], in_sem.at[i]
        )
        for i, (e, h, n) in enumerate(steps)
    ]
    outs = [
        pltpu.make_async_copy(
            made.at[i], out.at[e, :, pl.ds(h * HALF + n * PIECE, PIECE)], out_sem.at[i]
        )
        for i, (e, h, n) in enumerate(steps)
    ]
    for copy in ins:
        copy.start()
    line = lax.broadcasted_iota(jnp.int32, (WINDOW, 192), 0)
    for e in range(2):
        totals[e] = starts[8 + e, 0]
    for i, (e, h, n) in enumerate(steps):
        windows = [
            pl.multiple_of(jnp.minimum(starts[e * 4 + yy, 0] // 16 * 16, LINES - WINDOW), 16)
            for yy in range(4)
        ]
        if n == 0:
            for yy in range(4):
                mine = (h * 2 + e) * 4 + yy
                wanted = goal[mine : mine + 1, 0:192] - windows[yy]
                placer[yy] = jnp.where(wanted == line, 1.0, 0.0).astype(jnp.bfloat16)
        made[i, 192:] = jnp.zeros((LINES - 192, PIECE), jnp.bfloat16)
        ins[i].wait()
        for yy in range(4):
            part = jnp.dot(
                placer[yy], got[i, yy * 192 : (yy + 1) * 192, :], preferred_element_type=jnp.float32
            ).astype(jnp.bfloat16)
            if yy == 0:
                made[i, 0:WINDOW, :] = part
            else:
                shared = pl.ds(windows[yy], 16)
                made[i, shared, :] = made[i, shared, :] + part[:16]
                made[i, pl.ds(pl.multiple_of(windows[yy] + 16, 16), WINDOW - 16), :] = part[16:]
        outs[i].start()
    for copy in outs:
        copy.wait()


def shards(tokens, expert_ids):
    anywhere = pl.BlockSpec(memory_space=pl.ANY)
    vmem = pl.BlockSpec(memory_space=pltpu.VMEM)
    arrived, goal, starts, *_ = pl.pallas_call(
        exchange,
        out_shape=(
            jax.ShapeDtypeStruct((2, 2, LINES, HALF), jnp.bfloat16),
            jax.ShapeDtypeStruct((16, 256), jnp.int32),
            jax.ShapeDtypeStruct((16, TOK), jnp.int32),
            jax.ShapeDtypeStruct((2, 8, 2 * TOK, QUARTER), jnp.bfloat16),
            jax.ShapeDtypeStruct((2, 4, 3, 2, 2, 48, PIECE), jnp.bfloat16),
            jax.ShapeDtypeStruct((2, 4, 2, 2, 2, 48, PIECE), jnp.bfloat16),
        ),
        in_specs=[anywhere, vmem],
        out_specs=(anywhere, vmem, vmem, anywhere, anywhere, anywhere),
        scratch_shapes=[
            pltpu.VMEM((2, 8, 2 * TOK, QUARTER), jnp.bfloat16),
            pltpu.VMEM((2, 2, 16, 96, 8 * TOK), jnp.bfloat16),
            pltpu.VMEM((2, 2, 2, 16, 2, 48, PIECE), jnp.bfloat16),
            pltpu.VMEM((256, TOK), jnp.float32),
            pltpu.VMEM((256, TOK), jnp.float32),
            pltpu.VMEM((2, 16, TOP, TOK), jnp.int32),
            pltpu.VMEM((8, 8, TOK), jnp.float32),
            pltpu.VMEM((8, 8, TOK), jnp.float32),
            pltpu.SemaphoreType.DMA((2,)),
            pltpu.SemaphoreType.DMA((2,)),
            pltpu.SemaphoreType.DMA((2,)),
            pltpu.SemaphoreType.DMA((2,)),
            pltpu.SemaphoreType.DMA((2, 16)),
            pltpu.SemaphoreType.DMA((2, 16)),
            pltpu.SemaphoreType.DMA((2, 2, 3, 3, 2)),
            pltpu.SemaphoreType.DMA((2, 2, 3, 3, 2)),
            pltpu.SemaphoreType.DMA((2, 2, 3, 4)),
            pltpu.SemaphoreType.DMA((2, 2, 3, 4)),
            pltpu.SemaphoreType.DMA((8,)),
            pltpu.SemaphoreType.DMA((8,)),
            pltpu.SemaphoreType.DMA((2, 4, 3)),
            pltpu.SemaphoreType.DMA((2, 4, 3)),
            pltpu.SemaphoreType.DMA((2, 4, 2)),
            pltpu.SemaphoreType.DMA((2, 4, 2)),
            pltpu.SemaphoreType.DMA((2, 4, 16)),
            pltpu.SemaphoreType.DMA((2, 4, 16)),
            pltpu.SemaphoreType.DMA((2, 4)),
            pltpu.SemaphoreType.DMA((2, 2, 2)),
        ],
        compiler_params=pltpu.CompilerParams(
            collective_id=0, has_side_effects=True, vmem_limit_bytes=60 * 1024 * 1024
        ),
        name="exchange",
    )(tokens, expert_ids.T)

    return pl.pallas_call(
        place,
        out_shape=(
            jax.ShapeDtypeStruct((2, LINES, WIDTH), jnp.bfloat16),
            jax.ShapeDtypeStruct((2,), jnp.int32),
        ),
        in_specs=[pl.BlockSpec(memory_space=pltpu.SMEM), vmem, anywhere],
        out_specs=(anywhere, pl.BlockSpec(memory_space=pltpu.SMEM)),
        scratch_shapes=[
            pltpu.VMEM((4, WINDOW, 192), jnp.bfloat16),
            pltpu.VMEM((16, LINES, PIECE), jnp.bfloat16),
            pltpu.VMEM((16, LINES, PIECE), jnp.bfloat16),
            pltpu.SemaphoreType.DMA((16,)),
            pltpu.SemaphoreType.DMA((16,)),
        ],
        compiler_params=pltpu.CompilerParams(vmem_limit_bytes=60 * 1024 * 1024),
        name="place",
    )(starts, goal, arrived)


def solution(mesh):
    in_specs = (P("ep", None), P("ep", None))
    out_specs = (P("ep", None, None), P("ep"))
    return jax.shard_map(shards, mesh=mesh, in_specs=in_specs, out_specs=out_specs, check_vma=False)
```
